32 devices in a mesh: dp: 1 (over z), tp: 4 (over y), sp: 8 (over x, core).
Axes of the slice: x: 4, y: 4, z: 1, core: 2. Of those that a mesh axis runs over, the one named last changes fastest.
The devices are a block of a 4x4x8 slice.
Arguments:
- tokens: bfloat16 [16384, 768], P(('dp', 'sp'))
- glob_pos: int32 [1024], P('dp')
- w_query: bfloat16 [768, 12, 64], P(None, 'tp')
- w_key: bfloat16 [768, 12, 64], P(None, 'tp')
- w_value: bfloat16 [768, 12, 64], P(None, 'tp')
- w_out: bfloat16 [12, 64, 768], P('tp')
- w_up: bfloat16 [768, 3072], P(None, 'tp')
- w_down: bfloat16 [3072, 768], P('tp')
Outputs:
- output: bfloat16 [16384, 768], P(('dp', 'sp'))
All inputs are finite; a program needn't handle non-finite values.
Results may differ from the reference program's by a relative error of at most 0.00772977.
Values are sent between devices in bfloat16 or wider.
A program may use at most 768 MiB of HBM per device.

```python
import jax
import jax.numpy as jnp
from jax import lax
import math

D = 768
HEADS = 12
FF = 3072
WIN = 256
SEQ = 16384
GLOB = 1024

HEAD = D // HEADS


def setup_inputs(seed: int = 0, part: int = 0) -> dict:
    root_key = jax.random.key(seed)
    weight_root, part_root = jax.random.split(root_key, 2)
    part_key = jax.random.fold_in(part_root, part)
    tok_key, pos_key = jax.random.split(part_key, 2)
    tokens = jax.random.normal(tok_key, (SEQ, D), jnp.float32).astype(jnp.bfloat16)
    inner_pos = jax.random.permutation(pos_key, SEQ - 2)[: GLOB - 2] + 1
    glob_pos = jnp.sort(jnp.concatenate([jnp.array([0, SEQ - 1], jnp.int32), inner_pos.astype(jnp.int32)]))
    w_keys = jax.random.split(weight_root, 7)
    qk_std = (2.0 / D) ** 0.5
    out_std = max(1.0, ((2 * WIN + GLOB) / 50.0) ** 0.5) / math.sqrt(D)
    w_query = (jax.random.normal(w_keys[0], (D, HEADS, HEAD), jnp.float32) * qk_std).astype(jnp.bfloat16)
    w_key = (jax.random.normal(w_keys[1], (D, HEADS, HEAD), jnp.float32) * qk_std).astype(jnp.bfloat16)
    w_value = (jax.random.normal(w_keys[2], (D, HEADS, HEAD), jnp.float32) / math.sqrt(D)).astype(jnp.bfloat16)
    w_out = (jax.random.normal(w_keys[3], (HEADS, HEAD, D), jnp.float32) * out_std).astype(jnp.bfloat16)
    w_up = (jax.random.normal(w_keys[4], (D, FF), jnp.float32) / math.sqrt(D)).astype(jnp.bfloat16)
    w_down = (jax.random.normal(w_keys[5], (FF, D), jnp.float32) / math.sqrt(FF)).astype(jnp.bfloat16)
    return {'tokens': tokens, 'glob_pos': glob_pos, 'w_query': w_query, 'w_key': w_key, 'w_value': w_value, 'w_out': w_out, 'w_up': w_up, 'w_down': w_down}


def reference(tokens, glob_pos, w_query, w_key, w_value, w_out, w_up, w_down):
    scale = 1.0 / math.sqrt(HEAD)
    q_rows = jnp.dot(tokens, w_query.reshape(D, D), preferred_element_type=jnp.float32).astype(jnp.bfloat16).reshape(SEQ, HEADS, HEAD)
    k_rows = jnp.dot(tokens, w_key.reshape(D, D), preferred_element_type=jnp.float32).astype(jnp.bfloat16).reshape(SEQ, HEADS, HEAD)
    v_rows = jnp.dot(tokens, w_value.reshape(D, D), preferred_element_type=jnp.float32).astype(jnp.bfloat16).reshape(SEQ, HEADS, HEAD)
    glob_flag = jnp.zeros((SEQ,), jnp.int32).at[glob_pos].set(1)
    pad_cfg = ((WIN, WIN), (0, 0), (0, 0))
    k_pad = jnp.pad(k_rows, pad_cfg)
    v_pad = jnp.pad(v_rows, pad_cfg)
    flag_pad = jnp.pad(glob_flag, (WIN, WIN))
    k_glob = k_rows[glob_pos].astype(jnp.float32)
    v_glob = v_rows[glob_pos].astype(jnp.float32)
    q_block = 128
    key_span = q_block + 2 * WIN

    def window_block(blk_index):
        start = blk_index * q_block
        q_blk = lax.dynamic_slice_in_dim(q_rows, start, q_block).astype(jnp.float32)
        k_blk = lax.dynamic_slice_in_dim(k_pad, start, key_span).astype(jnp.float32)
        v_blk = lax.dynamic_slice_in_dim(v_pad, start, key_span).astype(jnp.float32)
        f_blk = lax.dynamic_slice_in_dim(flag_pad, start, key_span)
        q_pos = start + jnp.arange(q_block)
        k_pos = start - WIN + jnp.arange(key_span)
        k_ok = (k_pos >= 0) & (k_pos < SEQ) & (f_blk == 0)
        allowed = (jnp.abs(q_pos[:, None] - k_pos[None, :]) <= WIN) & k_ok[None, :]
        s_win = jnp.einsum('qhe,khe->hqk', q_blk, k_blk) * scale
        s_win = jnp.where(allowed[None], s_win, -jnp.inf)
        s_glob = jnp.einsum('qhe,ghe->hqg', q_blk, k_glob) * scale
        prob_rows = jax.nn.softmax(jnp.concatenate([s_win, s_glob], axis=2), axis=2)
        prob_rows = prob_rows.astype(jnp.bfloat16).astype(jnp.float32)
        v_all = jnp.concatenate([v_blk, v_glob], axis=0)
        return jnp.einsum('hqk,khe->qhe', prob_rows, v_all).astype(jnp.bfloat16)

    o_rows = lax.map(window_block, jnp.arange(SEQ // q_block)).reshape(SEQ, HEADS, HEAD)
    q_heads = jnp.transpose(q_rows[glob_pos], (1, 0, 2))
    k_heads = jnp.transpose(k_rows, (1, 0, 2))
    v_heads = jnp.transpose(v_rows, (1, 0, 2))

    def glob_head(head_parts):
        q_head, k_head, v_head = head_parts
        scores = jnp.dot(q_head, k_head.T, preferred_element_type=jnp.float32) * scale
        prob_rows = jax.nn.softmax(scores, axis=1).astype(jnp.bfloat16)
        return jnp.dot(prob_rows, v_head, preferred_element_type=jnp.float32).astype(jnp.bfloat16)

    glob_out = jnp.transpose(lax.map(glob_head, (q_heads, k_heads, v_heads)), (1, 0, 2))
    o_rows = o_rows.at[glob_pos].set(glob_out)
    mixed = jnp.dot(o_rows.reshape(SEQ, D), w_out.reshape(D, D), preferred_element_type=jnp.float32)
    hidden = (tokens.astype(jnp.float32) + mixed).astype(jnp.bfloat16)
    gelu_rows = jax.nn.gelu(jnp.dot(hidden, w_up, preferred_element_type=jnp.float32), approximate=True).astype(jnp.bfloat16)
    down_sum = jnp.dot(gelu_rows, w_down, preferred_element_type=jnp.float32)
    return (hidden.astype(jnp.float32) + down_sum).astype(jnp.bfloat16)
```

```python
import functools
import math

import jax
import jax.numpy as jnp
from jax import lax
from jax.experimental import pallas as pl
from jax.experimental.pallas import tpu as pltpu
from jax.sharding import PartitionSpec as P

WIN = 256
NEG = -1e38
BQ = 256
F32 = jnp.float32
BF16 = jnp.bfloat16
MESH = pl.DeviceIdType.MESH
NT = (((1,), (1,)), ((), ()))
TN = (((0,), (0,)), ((), ()))


def remote(src, dst, send, recv, where):
    return pltpu.make_async_remote_copy(src_ref=src, dst_ref=dst, send_sem=send, recv_sem=recv, device_id=where, device_id_type=MESH)


def attention_kernel(dims, x_ref, pick_ref, wqv_ref, wk_ref, kpad_ref, gpos_ref, wcat_ref,
                     o_ref, wr_ref,
                     halo, rs_recv, xg, qT, k_aug, vT, qgT, kg_aug, vgT, m_w, l_w, acc_w, part, part_recv, og_all, og_ext, o_loc,
                     halo_s, halo_r, rs_s, rs_r, ag_s, ag_r, agd_s, agd_r, pt_s, pt_r, og_s, og_r, a2a_s, a2a_r, loc_s,
                     wy_s, wy_r, wf_s, wf_r, wx_s, wx_r, wd_s, wd_r):
    n_sp, n_tp, n_heads, hd = dims
    n_rows = x_ref.shape[0]
    width = n_heads * hd
    n_x = n_sp // 2
    n_blk = n_rows // BQ
    s = lax.axis_index('sp')
    t = lax.axis_index('tp')
    core = s % 2
    chip = s // 2
    G = gpos_ref.shape[1]
    per = G // (n_sp * n_tp)
    wrows = wcat_ref.shape[0] // n_sp
    half = (wrows // 32) * 16

    def sp(d):
        return (s + d + n_sp) % n_sp

    def tp(d):
        return (t + d + n_tp) % n_tp

    bar = pltpu.get_barrier_semaphore()
    n_peers = 0
    for d in range(1, n_sp):
        pl.semaphore_signal(bar, inc=1, device_id={'sp': sp(d)}, device_id_type=MESH)
        n_peers += 1
    for dt in range(1, n_tp):
        for dx in range(n_x):
            pl.semaphore_signal(bar, inc=1, device_id={'sp': sp(2 * dx), 'tp': tp(dt)}, device_id_type=MESH)
            n_peers += 1
    pl.semaphore_wait(bar, n_peers)

    rs = [remote(pick_ref.at[sp(d)], rs_recv.at[s], rs_s.at[d - 1], rs_r.at[d - 1], {'sp': sp(d)}) for d in range(1, n_sp)]
    for c in rs:
        c.start()
    halo_c = [remote(x_ref.at[pl.ds(n_rows - WIN, WIN)], halo.at[0], halo_s.at[0], halo_r.at[0], {'sp': sp(1)}),
              remote(x_ref.at[pl.ds(0, WIN)], halo.at[1], halo_s.at[1], halo_r.at[1], {'sp': sp(-1)})]
    for c in halo_c:
        c.start()

    def wslice(piece):
        return pl.ds(pl.multiple_of(piece * wrows, 16), wrows)

    pieces = [s, sp(2)]
    wy = []
    for i, piece in enumerate(pieces):
        for j, (d, slot) in enumerate(((-1, 0), (1, 2))):
            wy.append(remote(wcat_ref.at[wslice(piece)], wr_ref.at[slot, wslice(piece)], wy_s.at[2 * i + j], wy_r.at[2 * i + j], {'tp': tp(d)}))

    def start_wy():
        for c in wy:
            c.start()

    wf = []
    for i, piece in enumerate(pieces):
        lo = pl.ds(pl.multiple_of(piece * wrows, 16), half)
        hi = pl.ds(pl.multiple_of(piece * wrows + half, 16), wrows - half)
        wf.append(remote(wr_ref.at[0, lo], wr_ref.at[1, lo], wf_s.at[2 * i], wf_r.at[2 * i], {'tp': tp(-1)}))
        wf.append(remote(wr_ref.at[2, hi], wr_ref.at[1, hi], wf_s.at[2 * i + 1], wf_r.at[2 * i + 1], {'tp': tp(1)}))
    wx = [remote(wr_ref.at[:, wslice(s)], wr_ref.at[:, wslice(s)], wx_s.at[0], wx_r.at[0], {'sp': sp(2)}),
          remote(wr_ref.at[:, wslice(sp(2))], wr_ref.at[:, wslice(sp(2))], wx_s.at[1], wx_r.at[1], {'sp': sp(-2)})]
    wx_in = [remote(wr_ref.at[:, wslice(sp(-2))], wr_ref.at[:, wslice(sp(-2))], wx_s.at[0], wx_r.at[0], {'sp': sp(2)}),
             remote(wr_ref.at[:, wslice(sp(4))], wr_ref.at[:, wslice(sp(4))], wx_s.at[1], wx_r.at[1], {'sp': sp(-2)})]
    partner = 2 * chip + 1 - core
    wd = [remote(wr_ref.at[:, wslice(sp(2 * j))], wr_ref.at[:, wslice(sp(2 * j))], wd_s.at[j], wd_r.at[j], {'sp': partner}) for j in range(4)]
    wd_in = [remote(wr_ref.at[:, wslice((partner + 2 * j) % n_sp)], wr_ref.at[:, wslice((partner + 2 * j) % n_sp)], wd_s.at[j], wd_r.at[j], {'sp': partner}) for j in range(4)]

    def project(rows, kdst, vdst, qdst, kdst_row, vcol, qcol):
        qv = lax.dot_general(wqv_ref[...], rows, NT, preferred_element_type=F32).astype(BF16)
        kk = jnp.dot(rows, wk_ref[...], preferred_element_type=F32).astype(BF16)
        kdst[kdst_row, pl.ds(0, width)] = kk
        vdst[:, vcol] = qv[width:]
        if qdst is not None:
            qdst[:, qcol] = (qv[:width].astype(F32) * (1.0 / math.sqrt(hd))).astype(BF16)

    def proj_block(b, carry):
        base = pl.multiple_of(b * BQ, BQ)
        ext = pl.multiple_of(b * BQ + WIN, BQ)
        project(x_ref[pl.ds(base, BQ)], k_aug, vT, qT, pl.ds(ext, BQ), pl.ds(ext, BQ), pl.ds(base, BQ))
        return carry

    k_aug[:, pl.ds(width, hd)] = kpad_ref[...]
    kg_aug[:, pl.ds(width, hd)] = jnp.zeros((G, hd), BF16)
    lax.fori_loop(0, n_blk, proj_block, 0)

    for c in rs:
        c.wait_recv()
    mine = core * (n_x * n_tp) + t * n_x + chip
    rs_recv[s] = pick_ref[s]
    xg[mine] = jnp.sum(rs_recv[...].astype(F32), axis=0).astype(BF16)
    ag = []
    for dt in range(n_tp):
        for dx in range(n_x):
            if dt or dx:
                j = dt * n_x + dx - 1
                ag.append(remote(xg.at[mine], xg.at[mine], ag_s.at[j], ag_r.at[j], {'sp': sp(2 * dx), 'tp': tp(dt)}))
    for c in ag:
        c.start()
    start_wy()
    for c in halo_c:
        c.wait_recv()
    project(halo[0], k_aug, vT, None, pl.ds(0, WIN), pl.ds(0, WIN), None)
    project(halo[1], k_aug, vT, None, pl.ds(n_rows + WIN, WIN), pl.ds(n_rows + WIN, WIN), None)

    flag_rows = (lax.broadcasted_iota(jnp.int32, (hd, BQ), 0) == 0).astype(F32).astype(BF16)

    def q_cols(src, h, cols, biased):
        parts = [src[pl.ds(h * hd, hd), cols]]
        if h:
            parts.insert(0, jnp.zeros((h * hd, BQ), BF16))
        if h + 1 < n_heads:
            parts.append(jnp.zeros(((n_heads - 1 - h) * hd, BQ), BF16))
        parts.append(flag_rows if biased else jnp.zeros((hd, BQ), BF16))
        return jnp.concatenate(parts, axis=0)

    jj = lax.broadcasted_iota(jnp.int32, (WIN, BQ), 0)
    ii = lax.broadcasted_iota(jnp.int32, (WIN, BQ), 1)

    def window_block(b, carry):
        base = pl.multiple_of(b * BQ, BQ)
        for h in range(n_heads):
            sc = jnp.dot(k_aug[pl.ds(base, BQ + 2 * WIN)], q_cols(qT, h, pl.ds(base, BQ), True), preferred_element_type=F32)
            sc = jnp.concatenate([jnp.where(ii <= jj, sc[:WIN], NEG), sc[WIN:WIN + BQ], jnp.where(jj <= ii, sc[WIN + BQ:], NEG)], axis=0)
            mx = jnp.max(sc, axis=0, keepdims=True)
            e = jnp.exp(sc - mx)
            m_w[b, pl.ds(h, 1)] = mx
            l_w[b, pl.ds(h, 1)] = jnp.sum(e, axis=0, keepdims=True)
            acc_w[b, pl.ds(h * hd, hd)] = jnp.dot(vT[pl.ds(h * hd, hd), pl.ds(base, BQ + 2 * WIN)], e.astype(BF16), preferred_element_type=F32)
        return carry

    lax.fori_loop(0, n_blk, window_block, 0)

    for c in ag:
        c.wait_recv()
    n_half = n_x * n_tp
    agd = remote(xg.at[pl.ds(core * n_half, n_half)], xg.at[pl.ds(core * n_half, n_half)], agd_s.at[0], agd_r.at[0], {'sp': partner})
    agd_in = remote(xg.at[pl.ds((1 - core) * n_half, n_half)], xg.at[pl.ds((1 - core) * n_half, n_half)], agd_s.at[0], agd_r.at[0], {'sp': partner})
    agd.start()
    for c in wy:
        c.wait_recv()
    for c in wf:
        c.start()
    agd_in.wait_recv()
    gb = BQ // per
    for g in range(G // BQ):
        rows = xg[pl.ds(g * gb, gb)].reshape(BQ, x_ref.shape[1])
        cols = pl.ds(g * BQ, BQ)
        project(rows, kg_aug, vgT, qgT, cols, cols, cols)

    gper = G // n_sp

    def gq_block(g, carry):
        cols = pl.ds(pl.multiple_of(g * BQ, BQ), BQ)
        for h in range(n_heads):
            sc = jnp.dot(k_aug[pl.ds(WIN, n_rows)], q_cols(qgT, h, cols, False), preferred_element_type=F32)
            mx = jnp.max(sc, axis=0, keepdims=True)
            e = jnp.exp(sc - mx)
            ls = jnp.sum(e, axis=0, keepdims=True)
            ac = jnp.dot(vT[pl.ds(h * hd, hd), pl.ds(WIN, n_rows)], e.astype(BF16), preferred_element_type=F32)
            for q in range(BQ // gper):
                cc = slice(q * gper, (q + 1) * gper)
                dst = g * (BQ // gper) + q
                part[dst, pl.ds(h * hd, hd)] = ac[:, cc]
                part[dst, pl.ds(width + h, 1)] = mx[:, cc]
                part[dst, pl.ds(width + 8 + h, 1)] = ls[:, cc]
        return carry

    lax.fori_loop(0, G // BQ, gq_block, 0)
    pt = [remote(part.at[sp(d)], part_recv.at[s], pt_s.at[d - 1], pt_r.at[d - 1], {'sp': sp(d)}) for d in range(1, n_sp)]
    for c in pt:
        c.start()
    for c in wf:
        c.wait_recv()
    for c in wx:
        c.start()
    wd[0].start()
    wd[1].start()

    def glob_block(b, carry):
        base = pl.multiple_of(b * BQ, BQ)
        for h in range(n_heads):
            sc = jnp.dot(kg_aug[...], q_cols(qT, h, pl.ds(base, BQ), False), preferred_element_type=F32)
            m_old = m_w[b, pl.ds(h, 1)]
            mx = jnp.maximum(jnp.max(sc, axis=0, keepdims=True), m_old)
            e = jnp.exp(sc - mx)
            alpha = jnp.exp(m_old - mx)
            ls = jnp.sum(e, axis=0, keepdims=True) + l_w[b, pl.ds(h, 1)] * alpha
            ac = jnp.dot(vgT[pl.ds(h * hd, hd)], e.astype(BF16), preferred_element_type=F32) + acc_w[b, pl.ds(h * hd, hd)] * alpha
            acc_w[b, pl.ds(h * hd, hd)] = ac / ls
        return carry

    lax.fori_loop(0, n_blk, glob_block, 0)

    for c in pt:
        c.wait_recv()
    part_recv[s] = part[s]
    for h in range(n_heads):
        ms = part_recv[:, pl.ds(width + h, 1)]
        mx = jnp.max(ms, axis=0, keepdims=True)
        wt = jnp.exp(ms - mx)
        den = jnp.sum(part_recv[:, pl.ds(width + 8 + h, 1)] * wt, axis=0)
        num = jnp.sum(part_recv[:, pl.ds(h * hd, hd)] * wt, axis=0)
        og_all[s, pl.ds(h * hd, hd)] = (num / den).astype(BF16)
    og = [remote(og_all.at[s], og_all.at[s], og_s.at[d - 1], og_r.at[d - 1], {'sp': sp(d)}) for d in range(1, n_sp)]
    for c in og:
        c.start()
    for c in og:
        c.wait_recv()
    og_ext[pl.ds(width, 16)] = jnp.ones((16, G), BF16)
    for d in range(n_sp):
        og_ext[pl.ds(0, width), pl.ds(d * gper, gper)] = og_all[d]

    chunk = n_rows // n_tp
    per_chunk = chunk // BQ
    gpos = gpos_ref[...]

    def pick_block(b, carry):
        pos = s * n_rows + b * BQ + lax.broadcasted_iota(jnp.int32, (BQ, G), 0)
        hot = (pos == gpos).astype(F32).astype(BF16)
        sel = lax.dot_general(og_ext[...], hot, NT, preferred_element_type=F32)
        res = jnp.where(sel[width:width + 1] > 0.5, sel[:width], acc_w[b])
        o_loc[b // per_chunk, :, pl.ds(pl.multiple_of((b % per_chunk) * BQ, BQ), BQ)] = res.astype(BF16)
        return carry

    lax.fori_loop(0, n_blk, pick_block, 0)
    a2a = [remote(o_loc.at[tp(-r)], o_ref.at[r], a2a_s.at[r - 1], a2a_r.at[r - 1], {'tp': tp(-r)}) for r in range(1, n_tp)]
    for c in a2a:
        c.start()
    own = pltpu.make_async_copy(o_loc.at[t], o_ref.at[0], loc_s)
    own.start()
    for c in wx_in:
        c.wait_recv()
    wd[2].start()
    wd[3].start()
    own.wait()
    for c in a2a:
        c.wait_recv()
    for c in wd_in:
        c.wait_recv()
    for c in rs + halo_c + ag + [agd] + pt + og + a2a + wy + wf + wx + wd:
        c.wait_send()


def mlp_kernel(dims, x_ref, o_ref, wcat_ref, wr_ref, y_ref,
               xbuf, wbuf, y_s, y_r, f_s, f_r, ld):
    n_sp, n_tp, n_heads, hd = dims
    n_rows, D = x_ref.shape
    width = n_heads * hd
    ff = (wcat_ref.shape[0] // 64) * 0 + D
    t = lax.axis_index('tp')

    def tp(d):
        return (t + d + n_tp) % n_tp

    chunk = n_rows // n_tp
    hrows = chunk // 2
    loads = [pltpu.make_async_copy(x_ref.at[pl.ds(pl.multiple_of(t * chunk, chunk), chunk)], xbuf, ld.at[n_tp]),
             pltpu.make_async_copy(wcat_ref, wbuf.at[0], ld.at[0])]
    for r in range(1, n_tp):
        loads.append(pltpu.make_async_copy(wr_ref.at[r - 1], wbuf.at[r], ld.at[r]))
    for c in loads:
        c.start()
    bar = pltpu.get_barrier_semaphore()
    for d in range(1, n_tp):
        pl.semaphore_signal(bar, inc=1, device_id={'tp': tp(d)}, device_id_type=MESH)
    pl.semaphore_wait(bar, n_tp - 1)
    for c in loads:
        c.wait()

    def rows_of(d, p):
        return pl.ds(pl.multiple_of(tp(d) * chunk + p * hrows, hrows), hrows)

    first, fwd, first_in, fwd_in = [], [], [], []
    for p in range(2):
        for j, d in enumerate((-1, 1)):
            first.append(remote(y_ref.at[rows_of(0, p)], y_ref.at[rows_of(0, p)], y_s.at[2 * p + j], y_r.at[2 * p + j], {'tp': tp(d)}))
            first_in.append(remote(y_ref.at[rows_of(-d, p)], y_ref.at[rows_of(-d, p)], y_s.at[2 * p + j], y_r.at[2 * p + j], {'tp': tp(d)}))
    fwd = [remote(y_ref.at[rows_of(1, 0)], y_ref.at[rows_of(1, 0)], f_s.at[0], f_r.at[0], {'tp': tp(-1)}),
           remote(y_ref.at[rows_of(-1, 1)], y_ref.at[rows_of(-1, 1)], f_s.at[1], f_r.at[1], {'tp': tp(1)})]
    fwd_in = [remote(y_ref.at[rows_of(2, 0)], y_ref.at[rows_of(2, 0)], f_s.at[0], f_r.at[0], {'tp': tp(-1)}),
              remote(y_ref.at[rows_of(2, 1)], y_ref.at[rows_of(2, 1)], f_s.at[1], f_r.at[1], {'tp': tp(1)})]

    for p in range(2):
        cols = pl.ds(p * hrows, hrows)
        mixed = jnp.zeros((hrows, D), F32)
        for r in range(n_tp):
            mixed = mixed + lax.dot_general(o_ref[r, :, cols], wbuf[r, pl.ds(2 * ff, width)], TN, preferred_element_type=F32)
        hidden = (xbuf[cols].astype(F32) + mixed).astype(BF16)
        down = jnp.zeros((hrows, D), F32)
        for r in range(n_tp):
            z = jnp.dot(hidden, wbuf[r, pl.ds(0, ff)], preferred_element_type=F32)
            u = jax.nn.gelu(z, approximate=True).astype(BF16)
            down = down + jnp.dot(u, wbuf[r, pl.ds(ff, ff)], preferred_element_type=F32)
        y_ref[rows_of(0, p)] = (hidden.astype(F32) + down).astype(BF16)
        first[2 * p].start()
        first[2 * p + 1].start()
    first_in[0].wait_recv()
    fwd[0].start()
    first_in[3].wait_recv()
    fwd[1].start()
    first_in[1].wait_recv()
    first_in[2].wait_recv()
    for c in fwd_in:
        c.wait_recv()
    for c in first + fwd:
        c.wait_send()


def solution(mesh):
    n_sp, n_tp = mesh.shape['sp'], mesh.shape['tp']

    def device_layer(tokens, glob_pos, w_query, w_key, w_value, w_out, w_up, w_down):
        n_rows, D = tokens.shape
        n_heads, hd = w_query.shape[1], w_query.shape[2]
        width = n_heads * hd
        G = glob_pos.shape[0]
        n_x = n_sp // 2
        per = G // (n_sp * n_tp)
        dims = (n_sp, n_tp, n_heads, hd)
        first = lax.axis_index('sp') * n_rows
        t = lax.axis_index('tp')
        ext_rows = n_rows + 2 * WIN

        slots = glob_pos.reshape(2, n_tp, n_x, per)
        slots = lax.dynamic_index_in_dim(slots, t, 1, keepdims=False).transpose(1, 0, 2).reshape(n_sp * per)
        hot = (slots[:, None] - first == jnp.arange(n_rows)[None, :]).astype(BF16)
        pick = jnp.dot(hot, tokens, preferred_element_type=F32).astype(BF16).reshape(n_sp, per, D)

        ext_pos = first - WIN + jnp.arange(ext_rows)
        off = jnp.any(ext_pos[:, None] == glob_pos[None, :], axis=1) | (ext_pos < 0) | (ext_pos >= n_rows * n_sp)
        kpad = jnp.where(off[:, None] & (jnp.arange(hd)[None, :] == 0), NEG, 0.0).astype(BF16)

        flat = lambda w: w.reshape(D, width)
        wqv = jnp.concatenate([flat(w_query).T, flat(w_value).T], axis=0)
        wtot = 2 * D + width
        wpad = -wtot % (n_sp * 16)
        wcat = jnp.concatenate([w_up, w_down, w_out.reshape(width, D), jnp.zeros((wpad, D), BF16)], axis=0)

        vm = pl.BlockSpec(memory_space=pltpu.VMEM)
        anyspace = pl.BlockSpec(memory_space=pl.ANY)
        dma = pltpu.SemaphoreType.DMA
        n_blk = n_rows // BQ
        o_all, wr = pl.pallas_call(
            functools.partial(attention_kernel, dims),
            out_shape=[jax.ShapeDtypeStruct((n_tp, width, n_rows // n_tp), BF16),
                       jax.ShapeDtypeStruct((n_tp - 1,) + wcat.shape, BF16)],
            in_specs=[vm] * 6 + [anyspace],
            out_specs=[vm, anyspace],
            scratch_shapes=[
                pltpu.VMEM((2, WIN, D), BF16), pltpu.VMEM((n_sp, per, D), BF16), pltpu.VMEM((n_sp * n_tp, per, D), BF16),
                pltpu.VMEM((width, n_rows), BF16), pltpu.VMEM((ext_rows, width + hd), BF16), pltpu.VMEM((width, ext_rows), BF16),
                pltpu.VMEM((width, G), BF16), pltpu.VMEM((G, width + hd), BF16), pltpu.VMEM((width, G), BF16),
                pltpu.VMEM((n_blk, 8, BQ), F32), pltpu.VMEM((n_blk, 8, BQ), F32), pltpu.VMEM((n_blk, width, BQ), F32),
                pltpu.VMEM((n_sp, width + 16, G // n_sp), F32), pltpu.VMEM((n_sp, width + 16, G // n_sp), F32),
                pltpu.VMEM((n_sp, width, G // n_sp), BF16), pltpu.VMEM((width + 16, G), BF16),
                pltpu.VMEM((n_tp, width, n_rows // n_tp), BF16),
                dma((2,)), dma((2,)), dma((n_sp - 1,)), dma((n_sp - 1,)), dma((n_x * n_tp - 1,)), dma((n_x * n_tp - 1,)),
                dma((1,)), dma((1,)), dma((n_sp - 1,)), dma((n_sp - 1,)), dma((n_sp - 1,)), dma((n_sp - 1,)),
                dma((n_tp - 1,)), dma((n_tp - 1,)), dma,
                dma((4,)), dma((4,)), dma((4,)), dma((4,)), dma((2,)), dma((2,)), dma((4,)), dma((4,)),
            ],
            compiler_params=pltpu.CompilerParams(collective_id=0, has_side_effects=True, vmem_limit_bytes=60 * 1024 * 1024),
            name='attention',
        )(tokens, pick, wqv, flat(w_key), kpad, glob_pos.reshape(1, G), wcat)

        return pl.pallas_call(
            functools.partial(mlp_kernel, dims),
            out_shape=jax.ShapeDtypeStruct((n_rows, D), BF16),
            in_specs=[anyspace, vm, anyspace, anyspace],
            out_specs=vm,
            scratch_shapes=[
                pltpu.VMEM((n_rows // n_tp, D), BF16), pltpu.VMEM((n_tp,) + wcat.shape, BF16),
                dma((4,)), dma((4,)), dma((2,)), dma((2,)), dma((n_tp + 1,)),
            ],
            compiler_params=pltpu.CompilerParams(collective_id=1, has_side_effects=True, vmem_limit_bytes=60 * 1024 * 1024),
            name='mlp',
        )(tokens, o_all, wcat, wr)

    row_spec = P(('dp', 'sp'), None)
    head_spec = P(None, 'tp', None)
    in_specs = (row_spec, P('dp'), head_spec, head_spec, head_spec, P('tp', None, None), P(None, 'tp'), P('tp', None))
    return jax.shard_map(device_layer, mesh=mesh, in_specs=in_specs, out_specs=row_spec, check_vma=False)
```

```python
import functools
import math

import jax
import jax.numpy as jnp
from jax import lax
from jax.experimental import pallas as pl
from jax.experimental.pallas import tpu as pltpu
from jax.sharding import PartitionSpec as P

WIN = 256
NEG = -1e38
LOG2E = math.log2(math.e)
BQ = 256
F32 = jnp.float32
BF16 = jnp.bfloat16
MESH = pl.DeviceIdType.MESH
NT = (((1,), (1,)), ((), ()))
TN = (((0,), (0,)), ((), ()))


def remote(src, dst, send, recv, where):
    return pltpu.make_async_remote_copy(src_ref=src, dst_ref=dst, send_sem=send, recv_sem=recv, device_id=where, device_id_type=MESH)


def layer_kernel(dims, x_ref, wqv_ref, wk_ref, scol_ref, gpos_ref, w1_ref, w2_ref, wo_ref,
                 y_ref,
                 w1_in, w2_in, wo_in, pick, halo, rs_recv, xg, s_scr, m_scr, qT, k_aug, vT, qgT, kg_aug, vgT, m_w, l_w, acc_w, part, part_recv,
                 og_all, og_ext, o_loc, o_in,
                 halo_s, halo_r, rs_s, rs_r, ag_s, ag_r, agd_s, agd_r, pt_s, pt_r, og_s, og_r, a2a_s, a2a_r,
                 wy_s, wy_r, wf_s, wf_r, wx_s, wx_r, wd_s, wd_r, y_s, y_r, f_s, f_r):
    n_sp, n_tp, n_heads, hd = dims
    n_rows, D = x_ref.shape
    width = n_heads * hd
    n_x = n_sp // 2
    n_blk = n_rows // BQ
    s = lax.axis_index('sp')
    t = lax.axis_index('tp')
    core = s % 2
    chip = s // 2
    G = gpos_ref.shape[1]
    per = G // (n_sp * n_tp)
    wrows = D // n_sp

    def sp(d):
        return (s + d + n_sp) % n_sp

    def tp(d):
        return (t + d + n_tp) % n_tp

    bar = pltpu.get_barrier_semaphore()
    n_peers = 0
    for d in range(1, n_sp):
        pl.semaphore_signal(bar, inc=1, device_id={'sp': sp(d)}, device_id_type=MESH)
        n_peers += 1
    for dt in range(1, n_tp):
        for dx in range(n_x):
            pl.semaphore_signal(bar, inc=1, device_id={'sp': sp(2 * dx), 'tp': tp(dt)}, device_id_type=MESH)
            n_peers += 1
    pl.semaphore_wait(bar, n_peers)

    halo_c = [remote(x_ref.at[pl.ds(n_rows - WIN, WIN)], halo.at[0], halo_s.at[0], halo_r.at[0], {'sp': sp(1)}),
              remote(x_ref.at[pl.ds(0, WIN)], halo.at[1], halo_s.at[1], halo_r.at[1], {'sp': sp(-1)})]
    for c in halo_c:
        c.start()

    weights = [(w1_ref, w1_in), (wo_ref, wo_in), (w2_ref, w2_in)]

    def wslice(piece):
        return pl.ds(pl.multiple_of(((piece + n_sp) % n_sp) * wrows, wrows), wrows)

    wy, wf, wx, wx_in, wd, wd_in = [], [], [], [], [], []
    partner = 2 * chip + 1 - core
    for p in range(2):
        rows = wslice(s + 2 * p)
        wy.append([remote(w.at[rows], win.at[slot, rows], wy_s.at[p, k, a], wy_r.at[p, k, a], {'tp': tp(d)})
                   for k, (d, slot) in enumerate(((-1, 0), (1, 2))) for a, (w, win) in enumerate(weights)])
        wf.append([remote(win.at[slot, rows], win.at[1, rows], wf_s.at[p, a], wf_r.at[p, a], {'tp': tp(d)})
                   for a, ((w, win), slot, d) in enumerate(zip(weights, (0, 0, 2), (-1, -1, 1)))])
        come = wslice(s - 2 if p == 0 else s + 4)
        wx.append([remote(win.at[:, rows], win.at[:, rows], wx_s.at[p, a], wx_r.at[p, a], {'sp': sp(2 - 4 * p)}) for a, (w, win) in enumerate(weights)])
        wx_in.append([remote(win.at[:, come], win.at[:, come], wx_s.at[p, a], wx_r.at[p, a], {'sp': sp(2 - 4 * p)}) for a, (w, win) in enumerate(weights)])
    for j in range(4):
        rows, come = wslice(s + 2 * j), wslice(partner + 2 * j)
        wd.append([remote(win.at[:, rows], win.at[:, rows], wd_s.at[j, a], wd_r.at[j, a], {'sp': partner}) for a, (w, win) in enumerate(weights)])
        wd_in.append([remote(win.at[:, come], win.at[:, come], wd_s.at[j, a], wd_r.at[j, a], {'sp': partner}) for a, (w, win) in enumerate(weights)])

    def start(copies):
        for c in copies:
            c.start()

    def arrive(copies):
        for c in copies:
            c.wait_recv()

    start(wy[0])

    hot = (s * n_rows + lax.broadcasted_iota(jnp.int32, (n_sp * per, n_rows), 1) == scol_ref[...]).astype(F32).astype(BF16)
    pick[...] = jnp.dot(hot, x_ref[...], preferred_element_type=F32).astype(BF16).reshape(n_sp, per, D)

    rs = [remote(pick.at[sp(d)], rs_recv.at[s], rs_s.at[d - 1], rs_r.at[d - 1], {'sp': sp(d)}) for d in range(1, n_sp)]
    start(rs)

    def project(rows, pad, kdst, vdst, qdst, kdst_row, vcol, qcol):
        qv = lax.dot_general(wqv_ref[...], rows, NT, preferred_element_type=F32).astype(BF16)
        kk = jnp.dot(rows, wk_ref[...], preferred_element_type=F32).astype(BF16)
        vdst[:, vcol] = qv[width:]
        for h in range(n_heads):
            kh = kk[:, h * hd:(h + 1) * hd]
            kdst[h, kdst_row, pl.ds(0, 2 * hd)] = jnp.concatenate([kh, kh], axis=1)
            kdst[h, kdst_row, pl.ds(2 * hd, 2 * hd)] = jnp.concatenate([kh, pad], axis=1)
        if qdst is not None:
            rest = qv[:width].astype(F32) * (LOG2E / math.sqrt(hd))
            for i in range(3):
                cut = rest.astype(BF16)
                rest = rest - cut.astype(F32)
                for h in range(n_heads):
                    qdst[h, pl.ds(i * hd, hd), qcol] = cut[h * hd:(h + 1) * hd]

    gpos = gpos_ref[...]
    mark = jnp.where(lax.broadcasted_iota(jnp.int32, (G, hd), 1) == 0, NEG, 0.0).astype(BF16)

    def key_pad(off):
        pos = s * n_rows + off + lax.broadcasted_iota(jnp.int32, (BQ, G), 0)
        pad = jnp.dot((pos == gpos).astype(F32).astype(BF16), mark, preferred_element_type=F32)
        at = s * n_rows + off + lax.broadcasted_iota(jnp.int32, (BQ, hd), 0)
        lane = lax.broadcasted_iota(jnp.int32, (BQ, hd), 1)
        return jnp.where((lane == 0) & ((at < 0) | (at >= n_rows * n_sp)), NEG, pad).astype(BF16)

    def proj_block(b, carry):
        base = pl.multiple_of(b * BQ, BQ)
        ext = pl.multiple_of(b * BQ + WIN, BQ)
        project(x_ref[pl.ds(base, BQ)], key_pad(base), k_aug, vT, qT, pl.ds(ext, BQ), pl.ds(ext, BQ), pl.ds(base, BQ))
        return carry

    flag_row = (lax.broadcasted_iota(jnp.int32, (hd, BQ), 0) == 0).astype(F32).astype(BF16)
    for h in range(n_heads):
        for b in range(n_blk):
            qT[h, pl.ds(3 * hd, hd), pl.ds(b * BQ, BQ)] = flag_row
        qgT[h, pl.ds(3 * hd, hd)] = jnp.zeros((hd, G), BF16)
    lax.fori_loop(0, n_blk, proj_block, 0)

    for c in rs:
        c.wait_recv()
    mine = core * (n_x * n_tp) + t * n_x + chip
    rs_recv[s] = pick[s]
    xg[mine] = jnp.sum(rs_recv[...].astype(F32), axis=0).astype(BF16)
    ag = []
    for dt in range(n_tp):
        for dx in range(n_x):
            if dt or dx:
                j = dt * n_x + dx - 1
                ag.append(remote(xg.at[mine], xg.at[mine], ag_s.at[j], ag_r.at[j], {'sp': sp(2 * dx), 'tp': tp(dt)}))
    start(ag)
    arrive(wy[0])
    start(wf[0])
    start(wy[1])
    arrive(halo_c)
    project(halo[0], key_pad(-WIN), k_aug, vT, None, pl.ds(0, WIN), pl.ds(0, WIN), None)
    project(halo[1], key_pad(n_rows), k_aug, vT, None, pl.ds(n_rows + WIN, WIN), pl.ds(n_rows + WIN, WIN), None)

    jj = lax.broadcasted_iota(jnp.int32, (WIN, BQ), 0)
    ii = lax.broadcasted_iota(jnp.int32, (WIN, BQ), 1)

    def pipeline(n_blocks, n_ch, keys, queries, values, window, finish):
        def score(b, h, c, mx):
            sc = jnp.dot(keys(b, h, c), queries(b, h), preferred_element_type=F32)
            if window and c == 0:
                sc = jnp.where(ii <= jj, sc, NEG)
            if window and c == n_ch - 1:
                sc = jnp.where(jj <= ii, sc, NEG)
            s_scr[h, pl.ds(c * BQ, BQ)] = sc
            top = jnp.max(sc.reshape(BQ // 8, 8, BQ), axis=0)
            return top if mx is None else jnp.maximum(mx, top)

        def first(b, h):
            mx = None
            for c in range(n_ch):
                mx = score(b, h, c, mx)
            m_scr[h] = mx

        def both(b, h, b2, h2):
            mx = jnp.max(m_scr[h], axis=0, keepdims=True)
            mx = finish(b, h, mx, None, None, True)
            nxt, ls, ac = None, None, None
            for c in range(n_ch):
                nxt = score(b2, h2, c, nxt)
                e = jnp.exp2(s_scr[h, pl.ds(c * BQ, BQ)] - mx)
                le = jnp.sum(e.reshape(BQ // 8, 8, BQ), axis=0)
                ls = le if ls is None else ls + le
                pv = jnp.dot(values(b, h, c), e.astype(BF16), preferred_element_type=F32)
                ac = pv if ac is None else ac + pv
            m_scr[h2] = nxt
            finish(b, h, mx, jnp.sum(ls, axis=0, keepdims=True), ac, False)

        def body(b, carry):
            for h in range(n_heads):
                if h + 1 < n_heads:
                    both(b, h, b, h + 1)
                else:
                    both(b, h, jnp.minimum(b + 1, n_blocks - 1), 0)
            return carry

        first(0, 0)
        lax.fori_loop(0, n_blocks, body, 0)

    def cols_of(b):
        return pl.ds(pl.multiple_of(b * BQ, BQ), BQ)

    def rows_at(b, c, off=0):
        return pl.ds(pl.multiple_of(b * BQ + c * BQ + off, BQ), BQ)

    def window_done(b, h, mx, ls, ac, start):
        if start:
            return mx
        m_w[b, pl.ds(h, 1)] = mx
        l_w[b, pl.ds(h, 1)] = ls
        acc_w[b, pl.ds(h * hd, hd)] = ac

    pipeline(n_blk, 1 + 2 * WIN // BQ, lambda b, h, c: k_aug[h, rows_at(b, c)], lambda b, h: qT[h, :, cols_of(b)],
             lambda b, h, c: vT[pl.ds(h * hd, hd), rows_at(b, c)], True, window_done)

    for c in ag:
        c.wait_recv()
    n_half = n_x * n_tp
    agd = remote(xg.at[pl.ds(core * n_half, n_half)], xg.at[pl.ds(core * n_half, n_half)], agd_s.at[0], agd_r.at[0], {'sp': partner})
    agd_in = remote(xg.at[pl.ds((1 - core) * n_half, n_half)], xg.at[pl.ds((1 - core) * n_half, n_half)], agd_s.at[0], agd_r.at[0], {'sp': partner})
    agd.start()
    arrive(wf[0])
    start(wx[0])
    arrive(wy[1])
    start(wf[1])
    agd_in.wait_recv()
    gb = BQ // per
    for g in range(G // BQ):
        rows = xg[pl.ds(g * gb, gb)].reshape(BQ, x_ref.shape[1])
        cols = pl.ds(g * BQ, BQ)
        project(rows, jnp.zeros((BQ, hd), BF16), kg_aug, vgT, qgT, cols, cols, cols)

    gper = G // n_sp

    def gq_done(g, h, mx, ls, ac, start):
        if start:
            return mx
        for q in range(BQ // gper):
            cc = slice(q * gper, (q + 1) * gper)
            dst = g * (BQ // gper) + q
            part[dst, pl.ds(h * hd, hd)] = ac[:, cc]
            part[dst, pl.ds(width + h, 1)] = mx[:, cc]
            part[dst, pl.ds(width + 8 + h, 1)] = ls[:, cc]

    pipeline(G // BQ, n_rows // BQ, lambda b, h, c: k_aug[h, pl.ds(WIN + c * BQ, BQ)], lambda b, h: qgT[h, :, cols_of(b)],
             lambda b, h, c: vT[pl.ds(h * hd, hd), pl.ds(WIN + c * BQ, BQ)], False, gq_done)
    pt = [remote(part.at[sp(d)], part_recv.at[s], pt_s.at[d - 1], pt_r.at[d - 1], {'sp': sp(d)}) for d in range(1, n_sp)]
    for c in pt:
        c.start()
    arrive(wf[1])
    start(wx[1])
    start(wd[0])
    start(wd[1])

    def glob_done(b, h, mx, ls, ac, start):
        m_old = m_w[b, pl.ds(h, 1)]
        if start:
            return jnp.maximum(mx, m_old)
        alpha = jnp.exp2(m_old - mx)
        total = ls + l_w[b, pl.ds(h, 1)] * alpha
        acc_w[b, pl.ds(h * hd, hd)] = (ac + acc_w[b, pl.ds(h * hd, hd)] * alpha) / total

    pipeline(n_blk, G // BQ, lambda b, h, c: kg_aug[h, pl.ds(c * BQ, BQ)], lambda b, h: qT[h, :, cols_of(b)],
             lambda b, h, c: vgT[pl.ds(h * hd, hd), pl.ds(c * BQ, BQ)], False, glob_done)

    for c in pt:
        c.wait_recv()
    part_recv[s] = part[s]
    for h in range(n_heads):
        ms = part_recv[:, pl.ds(width + h, 1)]
        mx = jnp.max(ms, axis=0, keepdims=True)
        wt = jnp.exp2(ms - mx)
        den = jnp.sum(part_recv[:, pl.ds(width + 8 + h, 1)] * wt, axis=0)
        num = jnp.sum(part_recv[:, pl.ds(h * hd, hd)] * wt, axis=0)
        og_all[s, pl.ds(h * hd, hd)] = (num / den).astype(BF16)
    og = [remote(og_all.at[s], og_all.at[s], og_s.at[d - 1], og_r.at[d - 1], {'sp': sp(d)}) for d in range(1, n_sp)]
    for c in og:
        c.start()
    for c in og:
        c.wait_recv()
    og_ext[pl.ds(width, 16)] = jnp.ones((16, G), BF16)
    for d in range(n_sp):
        og_ext[pl.ds(0, width), pl.ds(d * gper, gper)] = og_all[d]

    chunk = n_rows // n_tp
    per_chunk = chunk // BQ
    a2a = []
    for p in range(per_chunk):
        def pick_block(ch, carry):
            b = ch * per_chunk + p
            pos = s * n_rows + b * BQ + lax.broadcasted_iota(jnp.int32, (BQ, G), 0)
            hot = (pos == gpos).astype(F32).astype(BF16)
            sel = lax.dot_general(og_ext[...], hot, NT, preferred_element_type=F32)
            o_loc[p, ch] = jnp.where(sel[width:width + 1] > 0.5, sel[:width], acc_w[b]).astype(BF16)
            return carry

        lax.fori_loop(0, n_tp, pick_block, 0)
        a2a.append([remote(o_loc.at[p, tp(-r)], o_in.at[p, r - 1], a2a_s.at[p, r - 1], a2a_r.at[p, r - 1], {'tp': tp(-r)}) for r in range(1, n_tp)])
        start(a2a[p])
    arrive(wx_in[0])
    start(wd[3])
    arrive(wx_in[1])
    start(wd[2])

    def rows_of(d, p):
        return pl.ds(pl.multiple_of(tp(d) * chunk + p * BQ, BQ), BQ)

    first, first_in = [], []
    for p in range(2):
        for j, d in enumerate((-1, 1)):
            first.append(remote(y_ref.at[rows_of(0, p)], y_ref.at[rows_of(0, p)], y_s.at[2 * p + j], y_r.at[2 * p + j], {'tp': tp(d)}))
            first_in.append(remote(y_ref.at[rows_of(-d, p)], y_ref.at[rows_of(-d, p)], y_s.at[2 * p + j], y_r.at[2 * p + j], {'tp': tp(d)}))
    fwd = [remote(y_ref.at[rows_of(1, 0)], y_ref.at[rows_of(1, 0)], f_s.at[0], f_r.at[0], {'tp': tp(-1)}),
           remote(y_ref.at[rows_of(-1, 1)], y_ref.at[rows_of(-1, 1)], f_s.at[1], f_r.at[1], {'tp': tp(1)})]
    fwd_in = [remote(y_ref.at[rows_of(2, 0)], y_ref.at[rows_of(2, 0)], f_s.at[0], f_r.at[0], {'tp': tp(-1)}),
              remote(y_ref.at[rows_of(2, 1)], y_ref.at[rows_of(2, 1)], f_s.at[1], f_r.at[1], {'tp': tp(1)})]

    for p in range(2):
        arrive(a2a[p])
        if p == 0:
            for group in wd_in:
                arrive(group)
        mixed = jnp.zeros((BQ, D), F32)
        for r in range(n_tp):
            o_r = o_loc[p, t] if r == 0 else o_in[p, r - 1]
            w = wo_ref[...] if r == 0 else wo_in[r - 1]
            mixed = mixed + lax.dot_general(o_r, w, (((0,), (1,)), ((), ())), preferred_element_type=F32)
        hidden = (x_ref[rows_of(0, p)].astype(F32) + mixed).astype(BF16)
        down = jnp.zeros((BQ, D), F32)
        for r in range(n_tp):
            z = jnp.dot(hidden, w1_ref[...] if r == 0 else w1_in[r - 1], preferred_element_type=F32)
            u = jax.nn.gelu(z, approximate=True).astype(BF16)
            down = down + jnp.dot(u, w2_ref[...] if r == 0 else w2_in[r - 1], preferred_element_type=F32)
        y_ref[rows_of(0, p)] = (hidden.astype(F32) + down).astype(BF16)
        first[2 * p].start()
        first[2 * p + 1].start()
    first_in[0].wait_recv()
    fwd[0].start()
    first_in[3].wait_recv()
    fwd[1].start()
    first_in[1].wait_recv()
    first_in[2].wait_recv()
    arrive(fwd_in)
    for c in rs + halo_c + ag + [agd] + pt + og + sum(a2a + wy + wf + wx + wd, []) + first + fwd:
        c.wait_send()


def solution(mesh):
    n_sp, n_tp = mesh.shape['sp'], mesh.shape['tp']

    def device_layer(tokens, glob_pos, w_query, w_key, w_value, w_out, w_up, w_down):
        n_rows, D = tokens.shape
        n_heads, hd = w_query.shape[1], w_query.shape[2]
        width = n_heads * hd
        G = glob_pos.shape[0]
        n_x = n_sp // 2
        per = G // (n_sp * n_tp)
        dims = (n_sp, n_tp, n_heads, hd)
        t = lax.axis_index('tp')
        ext_rows = n_rows + 2 * WIN

        slots = glob_pos.reshape(2, n_tp, n_x, per)
        slots = lax.dynamic_index_in_dim(slots, t, 1, keepdims=False).transpose(1, 0, 2).reshape(n_sp * per)
        flat = lambda w: w.reshape(D, width)
        wqv = jnp.concatenate([flat(w_query).T, flat(w_value).T], axis=0)
        vm = pl.BlockSpec(memory_space=pltpu.VMEM)
        dma = pltpu.SemaphoreType.DMA
        n_blk = n_rows // BQ
        return pl.pallas_call(
            functools.partial(layer_kernel, dims),
            out_shape=jax.ShapeDtypeStruct((n_rows, D), BF16),
            in_specs=[vm] * 8,
            out_specs=vm,
            scratch_shapes=[
                pltpu.VMEM((n_tp - 1,) + w_up.shape, BF16), pltpu.VMEM((n_tp - 1,) + w_down.shape, BF16), pltpu.VMEM((n_tp - 1, D, width), BF16),
                pltpu.VMEM((n_sp, per, D), BF16),
                pltpu.VMEM((2, WIN, D), BF16), pltpu.VMEM((n_sp, per, D), BF16), pltpu.VMEM((n_sp * n_tp, per, D), BF16),
                pltpu.VMEM((n_heads, n_rows, BQ), F32), pltpu.VMEM((n_heads, 8, BQ), F32),
                pltpu.VMEM((n_heads, 4 * hd, n_rows), BF16), pltpu.VMEM((n_heads, ext_rows, 4 * hd), BF16), pltpu.VMEM((width, ext_rows), BF16),
                pltpu.VMEM((n_heads, 4 * hd, G), BF16), pltpu.VMEM((n_heads, G, 4 * hd), BF16), pltpu.VMEM((width, G), BF16),
                pltpu.VMEM((n_blk, 8, BQ), F32), pltpu.VMEM((n_blk, 8, BQ), F32), pltpu.VMEM((n_blk, width, BQ), F32),
                pltpu.VMEM((n_sp, width + 16, G // n_sp), F32), pltpu.VMEM((n_sp, width + 16, G // n_sp), F32),
                pltpu.VMEM((n_sp, width, G // n_sp), BF16), pltpu.VMEM((width + 16, G), BF16),
                pltpu.VMEM((2, n_tp, width, BQ), BF16), pltpu.VMEM((2, n_tp - 1, width, BQ), BF16),
                dma((2,)), dma((2,)), dma((n_sp - 1,)), dma((n_sp - 1,)), dma((n_x * n_tp - 1,)), dma((n_x * n_tp - 1,)),
                dma((1,)), dma((1,)), dma((n_sp - 1,)), dma((n_sp - 1,)), dma((n_sp - 1,)), dma((n_sp - 1,)),
                dma((2, n_tp - 1)), dma((2, n_tp - 1)),
                dma((2, 2, 3)), dma((2, 2, 3)), dma((2, 3)), dma((2, 3)), dma((2, 3)), dma((2, 3)), dma((4, 3)), dma((4, 3)),
                dma((4,)), dma((4,)), dma((2,)), dma((2,)),
            ],
            compiler_params=pltpu.CompilerParams(collective_id=0, has_side_effects=True, vmem_limit_bytes=62 * 1024 * 1024),
            name='layer',
        )(tokens, wqv, flat(w_key), slots.reshape(-1, 1), glob_pos.reshape(1, G), w_up, w_down, w_out.reshape(width, D).T)

    row_spec = P(('dp', 'sp'), None)
    head_spec = P(None, 'tp', None)
    in_specs = (row_spec, P('dp'), head_spec, head_spec, head_spec, P('tp', None, None), P(None, 'tp'), P('tp', None))
    return jax.shard_map(device_layer, mesh=mesh, in_specs=in_specs, out_specs=row_spec, check_vma=False)
```

```python
import functools
import math

import jax
import jax.numpy as jnp
from jax import lax
from jax.experimental import pallas as pl
from jax.experimental.pallas import tpu as pltpu
from jax.sharding import PartitionSpec as P

WIN = 256
NEG = -1e38
LOG2E = math.log2(math.e)
BQ = 256
F32 = jnp.float32
BF16 = jnp.bfloat16
MESH = pl.DeviceIdType.MESH
NT = (((1,), (1,)), ((), ()))
TN = (((0,), (0,)), ((), ()))


def remote(src, dst, send, recv, where):
    return pltpu.make_async_remote_copy(src_ref=src, dst_ref=dst, send_sem=send, recv_sem=recv, device_id=where, device_id_type=MESH)


def layer_kernel(dims, x_ref, wqv_ref, wk_ref, gpos_ref, w1_ref, w2_ref, wo_ref,
                 y_ref,
                 w1_own, w2_own, wo_own, w1_in, w2_in, wo_in, pick, halo, rs_recv, xg, s_scr, m_scr, qT, k_aug, vT, qgT, kg_aug, vgT, m_w, l_w, acc_w, part, part_recv,
                 og_all, og_ext, o_loc, o_in,
                 halo_s, halo_r, rs_s, rs_r, ag_s, ag_r, agd_s, agd_r, pt_s, pt_r, og_s, og_r, a2a_s, a2a_r,
                 wy_s, wy_r, wf_s, wf_r, wx_s, wx_r, wd_s, wd_r, y_s, y_r, f_s, f_r, own_s):
    n_sp, n_tp, n_heads, hd = dims
    n_rows, D = x_ref.shape
    width = n_heads * hd
    n_x = n_sp // 2
    n_blk = n_rows // BQ
    s = lax.axis_index('sp')
    t = lax.axis_index('tp')
    core = s % 2
    chip = s // 2
    G = gpos_ref.shape[0] * gpos_ref.shape[1]
    gpos = jnp.concatenate([gpos_ref[pl.ds(i, 1)] for i in range(gpos_ref.shape[0])], axis=1)
    per = G // (n_sp * n_tp)
    def sp(d):
        return (s + d + n_sp) % n_sp

    def tp(d):
        return (t + d + n_tp) % n_tp

    own = [pltpu.make_async_copy(a, b, own_s.at[i]) for i, (a, b) in enumerate(((wo_ref, wo_own), (w1_ref, w1_own), (w2_ref, w2_own)))]
    for c in own:
        c.start()

    bar = pltpu.get_barrier_semaphore()
    n_peers = 0
    for d in range(1, n_sp):
        pl.semaphore_signal(bar, inc=1, device_id={'sp': sp(d)}, device_id_type=MESH)
        n_peers += 1
    for dt in range(1, n_tp):
        for dx in range(n_x):
            pl.semaphore_signal(bar, inc=1, device_id={'sp': sp(2 * dx), 'tp': tp(dt)}, device_id_type=MESH)
            n_peers += 1
    pl.semaphore_wait(bar, n_peers)

    halo_c = [remote(x_ref.at[pl.ds(n_rows - WIN, WIN)], halo.at[0], halo_s.at[0], halo_r.at[0], {'sp': sp(1)}),
              remote(x_ref.at[pl.ds(0, WIN)], halo.at[1], halo_s.at[1], halo_r.at[1], {'sp': sp(-1)})]
    for c in halo_c:
        c.start()

    weights = [(wo_ref, wo_in, 2 * width // n_sp, 2), (w1_ref, w1_in, D // n_sp, 1), (w2_ref, w2_in, D // n_sp, 1)]

    def wslice(piece, size, share):
        return pl.ds(pl.multiple_of((((piece + n_sp) % n_sp) // share) * size, size), size)

    wy, wf, wxa, wxa_in, wxb, wxb_in, wd, wd_in = [], [], [], [], [], [], [], []
    partner = 2 * chip + 1 - core
    for p in range(2):
        gy, gf, ga, ga_in, gb2, gb_in = [], [], [], [], [], []
        d2 = {'sp': sp(2 - 4 * p)}
        for a, (w, win, size, share) in enumerate(weights):
            rows = wslice(s + 2 * p, size, share)
            come = wslice(s - 2 if p == 0 else s + 4, size, share)
            for k, (d, slot) in enumerate(((-1, 0), (1, 2))):
                gy.append(remote(w.at[rows], win.at[slot, rows], wy_s.at[p, k, a], wy_r.at[p, k, a], {'tp': tp(d)}))
                ga.append(remote(win.at[slot, rows], win.at[slot, rows], wx_s.at[p, k, a], wx_r.at[p, k, a], d2))
                ga_in.append(remote(win.at[slot, come], win.at[slot, come], wx_s.at[p, k, a], wx_r.at[p, k, a], d2))
            d, slot = ((-1, 0), (-1, 0), (1, 2))[a]
            gf.append(remote(win.at[slot, rows], win.at[1, rows], wf_s.at[p, a], wf_r.at[p, a], {'tp': tp(d)}))
            gb2.append(remote(win.at[1, rows], win.at[1, rows], wx_s.at[p, 2, a], wx_r.at[p, 2, a], d2))
            gb_in.append(remote(win.at[1, come], win.at[1, come], wx_s.at[p, 2, a], wx_r.at[p, 2, a], d2))
        wy.append(gy)
        wf.append(gf)
        wxa.append(ga)
        wxa_in.append(ga_in)
        wxb.append(gb2)
        wxb_in.append(gb_in)
    for j in range(4):
        gd, gd_in = [], []
        for a, (w, win, size, share) in enumerate(weights[1:]):
            rows, come = wslice(s + 2 * j, size, share), wslice(partner + 2 * j, size, share)
            gd.append(remote(win.at[:, rows], win.at[:, rows], wd_s.at[j, a], wd_r.at[j, a], {'sp': partner}))
            gd_in.append(remote(win.at[:, come], win.at[:, come], wd_s.at[j, a], wd_r.at[j, a], {'sp': partner}))
        wd.append(gd)
        wd_in.append(gd_in)

    def start(copies):
        for c in copies:
            c.start()

    def arrive(copies):
        for c in copies:
            c.wait_recv()

    start(wy[0])

    slots = jnp.concatenate([gpos_ref[pl.ds(c * n_tp + t, 1)] for c in range(2)], axis=1)
    slots = jnp.transpose(jnp.broadcast_to(slots, (8, n_sp * per)))[:, :1]
    hot = (s * n_rows + lax.broadcasted_iota(jnp.int32, (n_sp * per, n_rows), 1) == slots).astype(F32).astype(BF16)
    pick[...] = jnp.dot(hot, x_ref[...], preferred_element_type=F32).astype(BF16).reshape(n_sp, per, D)

    def slot_block(dev):
        return (dev % 2) * n_x + dev // 2

    rs = [remote(pick.at[slot_block(sp(d))], rs_recv.at[s], rs_s.at[d - 1], rs_r.at[d - 1], {'sp': sp(d)}) for d in range(1, n_sp)]
    start(rs)

    def project(rows, pad, kdst, vdst, qdst, kdst_row, vcol, qcol):
        qv = lax.dot_general(wqv_ref[...], rows, NT, preferred_element_type=F32).astype(BF16)
        kk = jnp.dot(rows, wk_ref[...], preferred_element_type=F32).astype(BF16)
        vdst[:, vcol] = qv[width:]
        for h in range(n_heads):
            kh = kk[:, h * hd:(h + 1) * hd]
            kdst[h, kdst_row, pl.ds(0, 2 * hd)] = jnp.concatenate([kh, kh], axis=1)
            kdst[h, kdst_row, pl.ds(2 * hd, 2 * hd)] = jnp.concatenate([kh, pad], axis=1)
        if qdst is not None:
            rest = qv[:width].astype(F32) * (LOG2E / math.sqrt(hd))
            for i in range(3):
                cut = rest.astype(BF16)
                rest = rest - cut.astype(F32)
                for h in range(n_heads):
                    qdst[h, pl.ds(i * hd, hd), qcol] = cut[h * hd:(h + 1) * hd]

    mark = jnp.where(lax.broadcasted_iota(jnp.int32, (G, hd), 1) == 0, NEG, 0.0).astype(BF16)

    def key_pad(off):
        pos = s * n_rows + off + lax.broadcasted_iota(jnp.int32, (BQ, G), 0)
        pad = jnp.dot((pos == gpos).astype(F32).astype(BF16), mark, preferred_element_type=F32)
        at = s * n_rows + off + lax.broadcasted_iota(jnp.int32, (BQ, hd), 0)
        lane = lax.broadcasted_iota(jnp.int32, (BQ, hd), 1)
        return jnp.where((lane == 0) & ((at < 0) | (at >= n_rows * n_sp)), NEG, pad).astype(BF16)

    def proj_block(b, carry):
        base = pl.multiple_of(b * BQ, BQ)
        ext = pl.multiple_of(b * BQ + WIN, BQ)
        project(x_ref[pl.ds(base, BQ)], key_pad(base), k_aug, vT, qT, pl.ds(ext, BQ), pl.ds(ext, BQ), pl.ds(base, BQ))
        return carry

    flag_row = (lax.broadcasted_iota(jnp.int32, (hd, BQ), 0) == 0).astype(F32).astype(BF16)
    for h in range(n_heads):
        for b in range(n_blk):
            qT[h, pl.ds(3 * hd, hd), pl.ds(b * BQ, BQ)] = flag_row
        qgT[h, pl.ds(3 * hd, hd)] = jnp.zeros((hd, G), BF16)
    lax.fori_loop(0, n_blk, proj_block, 0)

    for c in rs:
        c.wait_recv()
    mine = core * (n_x * n_tp) + t * n_x + chip
    rs_recv[s] = pick[core * n_x + chip]
    xg[mine] = jnp.sum(rs_recv[...].astype(F32), axis=0).astype(BF16)
    ag = []
    for dt in range(n_tp):
        for dx in range(n_x):
            if dt or dx:
                j = dt * n_x + dx - 1
                ag.append(remote(xg.at[mine], xg.at[mine], ag_s.at[j], ag_r.at[j], {'sp': sp(2 * dx), 'tp': tp(dt)}))
    start(ag)
    arrive(wy[0])
    start(wf[0])
    start(wxa[0])
    start(wy[1])
    arrive(halo_c)
    project(halo[0], key_pad(-WIN), k_aug, vT, None, pl.ds(0, WIN), pl.ds(0, WIN), None)
    project(halo[1], key_pad(n_rows), k_aug, vT, None, pl.ds(n_rows + WIN, WIN), pl.ds(n_rows + WIN, WIN), None)

    jj = lax.broadcasted_iota(jnp.int32, (WIN, BQ), 0)
    ii = lax.broadcasted_iota(jnp.int32, (WIN, BQ), 1)

    def pipeline(n_blocks, n_ch, keys, queries, values, window, finish, hooks=None):
        def score(b, h, c, mx):
            sc = jnp.dot(keys(b, h, c), queries(b, h), preferred_element_type=F32)
            if window and c == 0:
                sc = jnp.where(ii <= jj, sc, NEG)
            if window and c == n_ch - 1:
                sc = jnp.where(jj <= ii, sc, NEG)
            s_scr[h, pl.ds(c * BQ, BQ)] = sc
            top = jnp.max(sc.reshape(BQ // 8, 8, BQ), axis=0)
            return top if mx is None else jnp.maximum(mx, top)

        def first(b, h):
            mx = None
            for c in range(n_ch):
                mx = score(b, h, c, mx)
            m_scr[h] = mx

        def both(b, h, b2, h2):
            mx = jnp.max(m_scr[h], axis=0, keepdims=True)
            mx = finish(b, h, mx, None, None, True)
            nxt, ls, ac = None, None, None
            for c in range(n_ch):
                nxt = score(b2, h2, c, nxt)
                e = jnp.exp2(s_scr[h, pl.ds(c * BQ, BQ)] - mx)
                le = jnp.sum(e.reshape(BQ // 8, 8, BQ), axis=0)
                ls = le if ls is None else ls + le
                pv = jnp.dot(values(b, h, c), e.astype(BF16), preferred_element_type=F32)
                ac = pv if ac is None else ac + pv
            m_scr[h2] = nxt
            finish(b, h, mx, jnp.sum(ls, axis=0, keepdims=True), ac, False)

        def body(b, carry):
            for at, hook in (hooks or {}).items():
                pl.when(b == at)(hook)
            for h in range(n_heads):
                if h + 1 < n_heads:
                    both(b, h, b, h + 1)
                else:
                    both(b, h, jnp.minimum(b + 1, n_blocks - 1), 0)
            return carry

        first(0, 0)
        lax.fori_loop(0, n_blocks, body, 0)

    def cols_of(b):
        return pl.ds(pl.multiple_of(b * BQ, BQ), BQ)

    def rows_at(b, c, off=0):
        return pl.ds(pl.multiple_of(b * BQ + c * BQ + off, BQ), BQ)

    def window_done(b, h, mx, ls, ac, start):
        if start:
            return mx
        m_w[b, pl.ds(h, 1)] = mx
        l_w[b, pl.ds(h, 1)] = ls
        acc_w[b, pl.ds(h * hd, hd)] = ac

    pipeline(n_blk, 1 + 2 * WIN // BQ, lambda b, h, c: k_aug[h, rows_at(b, c)], lambda b, h: qT[h, :, cols_of(b)],
             lambda b, h, c: vT[pl.ds(h * hd, hd), rows_at(b, c)], True, window_done)

    for c in ag:
        c.wait_recv()
    n_half = n_x * n_tp
    agd = remote(xg.at[pl.ds(core * n_half, n_half)], xg.at[pl.ds(core * n_half, n_half)], agd_s.at[0], agd_r.at[0], {'sp': partner})
    agd_in = remote(xg.at[pl.ds((1 - core) * n_half, n_half)], xg.at[pl.ds((1 - core) * n_half, n_half)], agd_s.at[0], agd_r.at[0], {'sp': partner})
    agd.start()
    arrive(wf[0])
    start(wxb[0])
    start(wd[0])
    agd_in.wait_recv()
    gb = BQ // per
    for g in range(G // BQ):
        rows = xg[pl.ds(g * gb, gb)].reshape(BQ, x_ref.shape[1])
        cols = pl.ds(g * BQ, BQ)
        project(rows, jnp.zeros((BQ, hd), BF16), kg_aug, vgT, qgT, cols, cols, cols)

    gper = G // n_sp

    def second_piece():
        arrive(wy[1])
        start(wf[1])
        start(wxa[1])

    def gq_done(g, h, mx, ls, ac, start):
        if start:
            return mx
        for q in range(BQ // gper):
            cc = slice(q * gper, (q + 1) * gper)
            dst = g * (BQ // gper) + q
            part[dst, pl.ds(h * hd, hd)] = ac[:, cc]
            part[dst, pl.ds(width + h, 1)] = mx[:, cc]
            part[dst, pl.ds(width + 8 + h, 1)] = ls[:, cc]

    pipeline(G // BQ, n_rows // BQ, lambda b, h, c: k_aug[h, pl.ds(WIN + c * BQ, BQ)], lambda b, h: qgT[h, :, cols_of(b)],
             lambda b, h, c: vT[pl.ds(h * hd, hd), pl.ds(WIN + c * BQ, BQ)], False, gq_done, {1: second_piece})
    pt = [remote(part.at[sp(d)], part_recv.at[s], pt_s.at[d - 1], pt_r.at[d - 1], {'sp': sp(d)}) for d in range(1, n_sp)]
    for c in pt:
        c.start()
    def second_forward():
        arrive(wf[1])
        start(wxb[1])
        start(wd[1])

    def glob_done(b, h, mx, ls, ac, start):
        m_old = m_w[b, pl.ds(h, 1)]
        if start:
            return jnp.maximum(mx, m_old)
        alpha = jnp.exp2(m_old - mx)
        total = ls + l_w[b, pl.ds(h, 1)] * alpha
        acc_w[b, pl.ds(h * hd, hd)] = (ac + acc_w[b, pl.ds(h * hd, hd)] * alpha) / total

    pipeline(n_blk, G // BQ, lambda b, h, c: kg_aug[h, pl.ds(c * BQ, BQ)], lambda b, h: qT[h, :, cols_of(b)],
             lambda b, h, c: vgT[pl.ds(h * hd, hd), pl.ds(c * BQ, BQ)], False, glob_done, {2: second_forward})

    for c in pt:
        c.wait_recv()
    part_recv[s] = part[s]
    for h in range(n_heads):
        ms = part_recv[:, pl.ds(width + h, 1)]
        mx = jnp.max(ms, axis=0, keepdims=True)
        wt = jnp.exp2(ms - mx)
        den = jnp.sum(part_recv[:, pl.ds(width + 8 + h, 1)] * wt, axis=0)
        num = jnp.sum(part_recv[:, pl.ds(h * hd, hd)] * wt, axis=0)
        og_all[s, pl.ds(h * hd, hd)] = (num / den).astype(BF16)
    og = [remote(og_all.at[s], og_all.at[s], og_s.at[d - 1], og_r.at[d - 1], {'sp': sp(d)}) for d in range(1, n_sp)]
    for c in og:
        c.start()
    arrive(wxa_in[0])
    arrive(wxb_in[0])
    start(wd[3])
    for c in og:
        c.wait_recv()
    og_ext[pl.ds(width, 16)] = jnp.ones((16, G), BF16)
    for d in range(n_sp):
        og_ext[pl.ds(0, width), pl.ds(d * gper, gper)] = og_all[d]

    chunk = n_rows // n_tp
    per_chunk = chunk // BQ
    a2a = []
    for p in range(per_chunk):
        def pick_block(ch, carry):
            b = ch * per_chunk + p
            pos = s * n_rows + b * BQ + lax.broadcasted_iota(jnp.int32, (BQ, G), 0)
            hot = (pos == gpos).astype(F32).astype(BF16)
            sel = lax.dot_general(og_ext[...], hot, NT, preferred_element_type=F32)
            o_loc[p, ch] = jnp.where(sel[width:width + 1] > 0.5, sel[:width], acc_w[b]).astype(BF16)
            return carry

        lax.fori_loop(0, n_tp, pick_block, 0)
        a2a.append([remote(o_loc.at[p, tp(-r)], o_in.at[p, r - 1], a2a_s.at[p, r - 1], a2a_r.at[p, r - 1], {'tp': tp(-r)}) for r in range(1, n_tp)])
        start(a2a[p])
    arrive(wxa_in[1])
    arrive(wxb_in[1])
    start(wd[2])

    def rows_of(d, p):
        return pl.ds(pl.multiple_of(tp(d) * chunk + p * BQ, BQ), BQ)

    first, first_in = [], []
    for p in range(2):
        for j, d in enumerate((-1, 1)):
            first.append(remote(y_ref.at[rows_of(0, p)], y_ref.at[rows_of(0, p)], y_s.at[2 * p + j], y_r.at[2 * p + j], {'tp': tp(d)}))
            first_in.append(remote(y_ref.at[rows_of(-d, p)], y_ref.at[rows_of(-d, p)], y_s.at[2 * p + j], y_r.at[2 * p + j], {'tp': tp(d)}))
    fwd = [remote(y_ref.at[rows_of(1, 0)], y_ref.at[rows_of(1, 0)], f_s.at[0], f_r.at[0], {'tp': tp(-1)}),
           remote(y_ref.at[rows_of(-1, 1)], y_ref.at[rows_of(-1, 1)], f_s.at[1], f_r.at[1], {'tp': tp(1)})]
    fwd_in = [remote(y_ref.at[rows_of(2, 0)], y_ref.at[rows_of(2, 0)], f_s.at[0], f_r.at[0], {'tp': tp(-1)}),
              remote(y_ref.at[rows_of(2, 1)], y_ref.at[rows_of(2, 1)], f_s.at[1], f_r.at[1], {'tp': tp(1)})]

    for p in range(2):
        arrive(a2a[p])
        if p == 0:
            for c in own:
                c.wait()
            for group in wd_in:
                arrive(group)
        mixed = jnp.zeros((BQ, D), F32)
        for r in range(n_tp):
            o_r = o_loc[p, t] if r == 0 else o_in[p, r - 1]
            w = wo_own[...] if r == 0 else wo_in[r - 1]
            mixed = mixed + lax.dot_general(o_r, w, TN, preferred_element_type=F32)
        hidden = (x_ref[rows_of(0, p)].astype(F32) + mixed).astype(BF16)
        down = jnp.zeros((BQ, D), F32)
        for r in range(n_tp):
            z = jnp.dot(hidden, w1_own[...] if r == 0 else w1_in[r - 1], preferred_element_type=F32)
            u = jax.nn.gelu(z, approximate=True).astype(BF16)
            down = down + jnp.dot(u, w2_own[...] if r == 0 else w2_in[r - 1], preferred_element_type=F32)
        y_ref[rows_of(0, p)] = (hidden.astype(F32) + down).astype(BF16)
        first[2 * p].start()
        first[2 * p + 1].start()
    first_in[0].wait_recv()
    fwd[0].start()
    first_in[3].wait_recv()
    fwd[1].start()
    first_in[1].wait_recv()
    first_in[2].wait_recv()
    arrive(fwd_in)
    for c in rs + halo_c + ag + [agd] + pt + og + sum(a2a + wy + wf + wxa + wxb + wd, []) + first + fwd:
        c.wait_send()


def solution(mesh):
    n_sp, n_tp = mesh.shape['sp'], mesh.shape['tp']

    def device_layer(tokens, glob_pos, w_query, w_key, w_value, w_out, w_up, w_down):
        n_rows, D = tokens.shape
        n_heads, hd = w_query.shape[1], w_query.shape[2]
        width = n_heads * hd
        G = glob_pos.shape[0]
        n_x = n_sp // 2
        per = G // (n_sp * n_tp)
        dims = (n_sp, n_tp, n_heads, hd)
        ext_rows = n_rows + 2 * WIN

        flat = lambda w: w.reshape(D, width)
        wqv = jnp.concatenate([flat(w_query).T, flat(w_value).T], axis=0)
        vm = pl.BlockSpec(memory_space=pltpu.VMEM)
        dma = pltpu.SemaphoreType.DMA
        n_blk = n_rows // BQ
        return pl.pallas_call(
            functools.partial(layer_kernel, dims),
            out_shape=jax.ShapeDtypeStruct((n_rows, D), BF16),
            in_specs=[vm] * 4 + [pl.BlockSpec(memory_space=pl.ANY)] * 3,
            out_specs=vm,
            scratch_shapes=[
                pltpu.VMEM(w_up.shape, BF16), pltpu.VMEM(w_down.shape, BF16), pltpu.VMEM((width, D), BF16),
                pltpu.VMEM((n_tp - 1,) + w_up.shape, BF16), pltpu.VMEM((n_tp - 1,) + w_down.shape, BF16), pltpu.VMEM((n_tp - 1, width, D), BF16),
                pltpu.VMEM((n_sp, per, D), BF16),
                pltpu.VMEM((2, WIN, D), BF16), pltpu.VMEM((n_sp, per, D), BF16), pltpu.VMEM((n_sp * n_tp, per, D), BF16),
                pltpu.VMEM((n_heads, n_rows, BQ), F32), pltpu.VMEM((n_heads, 8, BQ), F32),
                pltpu.VMEM((n_heads, 4 * hd, n_rows), BF16), pltpu.VMEM((n_heads, ext_rows, 4 * hd), BF16), pltpu.VMEM((width, ext_rows), BF16),
                pltpu.VMEM((n_heads, 4 * hd, G), BF16), pltpu.VMEM((n_heads, G, 4 * hd), BF16), pltpu.VMEM((width, G), BF16),
                pltpu.VMEM((n_blk, 8, BQ), F32), pltpu.VMEM((n_blk, 8, BQ), F32), pltpu.VMEM((n_blk, width, BQ), F32),
                pltpu.VMEM((n_sp, width + 16, G // n_sp), F32), pltpu.VMEM((n_sp, width + 16, G // n_sp), F32),
                pltpu.VMEM((n_sp, width, G // n_sp), BF16), pltpu.VMEM((width + 16, G), BF16),
                pltpu.VMEM((2, n_tp, width, BQ), BF16), pltpu.VMEM((2, n_tp - 1, width, BQ), BF16),
                dma((2,)), dma((2,)), dma((n_sp - 1,)), dma((n_sp - 1,)), dma((n_x * n_tp - 1,)), dma((n_x * n_tp - 1,)),
                dma((1,)), dma((1,)), dma((n_sp - 1,)), dma((n_sp - 1,)), dma((n_sp - 1,)), dma((n_sp - 1,)),
                dma((2, n_tp - 1)), dma((2, n_tp - 1)),
                dma((2, 2, 3)), dma((2, 2, 3)), dma((2, 3)), dma((2, 3)), dma((2, 3, 3)), dma((2, 3, 3)), dma((4, 2)), dma((4, 2)),
                dma((4,)), dma((4,)), dma((2,)), dma((2,)), dma((3,)),
            ],
            compiler_params=pltpu.CompilerParams(collective_id=0, has_side_effects=True, vmem_limit_bytes=62 * 1024 * 1024),
            name='layer',
        )(tokens, wqv, flat(w_key), glob_pos.reshape(2 * n_tp, n_x * per), w_up, w_down, w_out.reshape(width, D))

    row_spec = P(('dp', 'sp'), None)
    head_spec = P(None, 'tp', None)
    in_specs = (row_spec, P('dp'), head_spec, head_spec, head_spec, P('tp', None, None), P(None, 'tp'), P('tp', None))
    return jax.shard_map(device_layer, mesh=mesh, in_specs=in_specs, out_specs=row_spec, check_vma=False)
```

```python
import functools
import math

import jax
import jax.numpy as jnp
from jax import lax
from jax.experimental import pallas as pl
from jax.experimental.pallas import tpu as pltpu
from jax.sharding import PartitionSpec as P

WIN = 256
NEG = -1e38
LOG2E = math.log2(math.e)
BQ = 256
F32 = jnp.float32
BF16 = jnp.bfloat16
MESH = pl.DeviceIdType.MESH
NT = (((1,), (1,)), ((), ()))
TN = (((0,), (0,)), ((), ()))


def remote(src, dst, send, recv, where):
    return pltpu.make_async_remote_copy(src_ref=src, dst_ref=dst, send_sem=send, recv_sem=recv, device_id=where, device_id_type=MESH)


def layer_kernel(dims, x_ref, wqkv_ref, gpos_ref, w1_ref, w2_ref, wo_ref,
                 y_ref,
                 w1_own, w2_own, wo_own, w1_in, w2_in, wo_in, pick, halo, rs_recv, xg, s_scr, m_scr, qT, k_aug, vT, qgT, kg_aug, vgT, m_w, l_w, acc_w, part, part_recv,
                 og_all, og_ext, o_loc, o_in,
                 halo_s, halo_r, rs_s, rs_r, ag_s, ag_r, agd_s, agd_r, pt_s, pt_r, og_s, og_r, a2a_s, a2a_r,
                 wy_s, wy_r, wf_s, wf_r, wx_s, wx_r, wd_s, wd_r, y_s, y_r, f_s, f_r, own_s):
    n_sp, n_tp, n_heads, hd = dims
    n_rows, D = x_ref.shape
    width = n_heads * hd
    n_x = n_sp // 2
    n_blk = n_rows // BQ
    s = lax.axis_index('sp')
    t = lax.axis_index('tp')
    core = s % 2
    chip = s // 2
    G = gpos_ref.shape[0] * gpos_ref.shape[1]
    gpos = jnp.concatenate([gpos_ref[pl.ds(i, 1)] for i in range(gpos_ref.shape[0])], axis=1)
    per = G // (n_sp * n_tp)
    def sp(d):
        return (s + d + n_sp) % n_sp

    def tp(d):
        return (t + d + n_tp) % n_tp

    own = [pltpu.make_async_copy(a, b, own_s.at[i]) for i, (a, b) in enumerate(((wo_ref, wo_own), (w1_ref, w1_own), (w2_ref, w2_own)))]
    for c in own:
        c.start()

    bar = pltpu.get_barrier_semaphore()
    n_peers = 0
    for d in range(1, n_sp):
        pl.semaphore_signal(bar, inc=1, device_id={'sp': sp(d)}, device_id_type=MESH)
        n_peers += 1
    for dt in range(1, n_tp):
        for dx in range(n_x):
            pl.semaphore_signal(bar, inc=1, device_id={'sp': sp(2 * dx), 'tp': tp(dt)}, device_id_type=MESH)
            n_peers += 1
    pl.semaphore_wait(bar, n_peers)

    halo_c = [remote(x_ref.at[pl.ds(n_rows - WIN, WIN)], halo.at[0], halo_s.at[0], halo_r.at[0], {'sp': sp(1)}),
              remote(x_ref.at[pl.ds(0, WIN)], halo.at[1], halo_s.at[1], halo_r.at[1], {'sp': sp(-1)})]
    for c in halo_c:
        c.start()

    weights = [(wo_ref, wo_in, 2 * width // n_sp, 2), (w1_ref, w1_in, D // n_sp, 1), (w2_ref, w2_in, D // n_sp, 1)]

    def wslice(piece, size, share):
        return pl.ds(pl.multiple_of((((piece + n_sp) % n_sp) // share) * size, size), size)

    wy, wf, wxa, wxa_in, wxb, wxb_in, wd, wd_in = [], [], [], [], [], [], [], []
    partner = 2 * chip + 1 - core
    for p in range(3):
        gy, gf, ga, ga_in, gb2, gb_in = [], [], [], [], [], []
        d2 = {'sp': sp(2 - 2 * p)}
        for a, (w, win, size, share) in enumerate(weights):
            rows = wslice(s + 2 * p, size, share)
            come = wslice(s - 2, size, share)
            for k, (d, slot) in enumerate(((-1, 0), (1, 2))):
                gy.append(remote(w.at[rows], win.at[slot, rows], wy_s.at[p, k, a], wy_r.at[p, k, a], {'tp': tp(d)}))
            d, slot = ((-1, 0), (-1, 0), (1, 2))[a]
            gf.append(remote(win.at[slot, rows], win.at[1, rows], wf_s.at[p, a], wf_r.at[p, a], {'tp': tp(d)}))
            if p == (0, 0, 2)[a]:
                for slot in (0, 2):
                    ga.append(remote(win.at[slot, rows], win.at[slot, rows], wx_s.at[slot, a], wx_r.at[slot, a], d2))
                    ga_in.append(remote(win.at[slot, come], win.at[slot, come], wx_s.at[slot, a], wx_r.at[slot, a], d2))
                gb2.append(remote(win.at[1, rows], win.at[1, rows], wx_s.at[1, a], wx_r.at[1, a], d2))
                gb_in.append(remote(win.at[1, come], win.at[1, come], wx_s.at[1, a], wx_r.at[1, a], d2))
        wy.append(gy)
        wf.append(gf)
        wxa.append(ga)
        wxa_in.append(ga_in)
        wxb.append(gb2)
        wxb_in.append(gb_in)
    for j in range(4):
        gd, gd_in = [], []
        for a, (w, win, size, share) in enumerate(weights[1:]):
            rows, come = wslice(s + 2 * j, size, share), wslice(partner + 2 * j, size, share)
            gd.append(remote(win.at[:, rows], win.at[:, rows], wd_s.at[j, a], wd_r.at[j, a], {'sp': partner}))
            gd_in.append(remote(win.at[:, come], win.at[:, come], wd_s.at[j, a], wd_r.at[j, a], {'sp': partner}))
        wd.append(gd)
        wd_in.append(gd_in)

    def start(copies):
        for c in copies:
            c.start()

    def arrive(copies):
        for c in copies:
            c.wait_recv()

    start(wy[0])

    slots = jnp.concatenate([gpos_ref[pl.ds(c * n_tp + t, 1)] for c in range(2)], axis=1)
    slots = jnp.transpose(jnp.broadcast_to(slots, (8, n_sp * per)))[:, :1]
    hot = (s * n_rows + lax.broadcasted_iota(jnp.int32, (n_sp * per, n_rows), 1) == slots).astype(F32).astype(BF16)
    pick[...] = jnp.dot(hot, x_ref[...], preferred_element_type=F32).astype(BF16).reshape(n_sp, per, D)

    def slot_block(dev):
        return (dev % 2) * n_x + dev // 2

    rs = [remote(pick.at[slot_block(sp(d))], rs_recv.at[s], rs_s.at[d - 1], rs_r.at[d - 1], {'sp': sp(d)}) for d in range(1, n_sp)]
    start(rs)

    def project(rows, pad, kdst, vdst, qdst, kdst_row, vcol, qcol):
        qv = lax.dot_general(wqkv_ref[pl.ds(0, 2 * width)], rows, NT, preferred_element_type=F32).astype(BF16)
        kk = lax.dot_general(rows, wqkv_ref[pl.ds(2 * width, width)], NT, preferred_element_type=F32).astype(BF16)
        vdst[:, vcol] = qv[width:]
        for h in range(n_heads):
            kh = kk[:, h * hd:(h + 1) * hd]
            kdst[h, kdst_row, pl.ds(0, 2 * hd)] = jnp.concatenate([kh, kh], axis=1)
            kdst[h, kdst_row, pl.ds(2 * hd, 2 * hd)] = jnp.concatenate([kh, pad], axis=1)
        if qdst is not None:
            rest = qv[:width].astype(F32) * (LOG2E / math.sqrt(hd))
            for i in range(3):
                cut = rest.astype(BF16)
                rest = rest - cut.astype(F32)
                for h in range(n_heads):
                    qdst[h, pl.ds(i * hd, hd), qcol] = cut[h * hd:(h + 1) * hd]

    mark = jnp.where(lax.broadcasted_iota(jnp.int32, (G, hd), 1) == 0, NEG, 0.0).astype(BF16)

    def key_pad(off):
        pos = s * n_rows + off + lax.broadcasted_iota(jnp.int32, (BQ, G), 0)
        pad = jnp.dot((pos == gpos).astype(F32).astype(BF16), mark, preferred_element_type=F32)
        at = s * n_rows + off + lax.broadcasted_iota(jnp.int32, (BQ, hd), 0)
        lane = lax.broadcasted_iota(jnp.int32, (BQ, hd), 1)
        return jnp.where((lane == 0) & ((at < 0) | (at >= n_rows * n_sp)), NEG, pad).astype(BF16)

    def proj_block(b, carry):
        base = pl.multiple_of(b * BQ, BQ)
        ext = pl.multiple_of(b * BQ + WIN, BQ)
        project(x_ref[pl.ds(base, BQ)], key_pad(base), k_aug, vT, qT, pl.ds(ext, BQ), pl.ds(ext, BQ), pl.ds(base, BQ))
        return carry

    flag_row = (lax.broadcasted_iota(jnp.int32, (hd, BQ), 0) == 0).astype(F32).astype(BF16)
    for h in range(n_heads):
        for b in range(n_blk):
            qT[h, pl.ds(3 * hd, hd), pl.ds(b * BQ, BQ)] = flag_row
        qgT[h, pl.ds(3 * hd, hd)] = jnp.zeros((hd, G), BF16)
    lax.fori_loop(0, n_blk, proj_block, 0)

    for c in rs:
        c.wait_recv()
    mine = core * (n_x * n_tp) + t * n_x + chip
    rs_recv[s] = pick[core * n_x + chip]
    xg[mine] = jnp.sum(rs_recv[...].astype(F32), axis=0).astype(BF16)
    ag = []
    for dt in range(n_tp):
        for dx in range(n_x):
            if dt or dx:
                j = dt * n_x + dx - 1
                ag.append(remote(xg.at[mine], xg.at[mine], ag_s.at[j], ag_r.at[j], {'sp': sp(2 * dx), 'tp': tp(dt)}))
    start(ag)
    arrive(wy[0])
    start(wf[0])
    start(wxa[0])
    start(wy[1])
    start(wy[2])
    arrive(halo_c)
    project(halo[0], key_pad(-WIN), k_aug, vT, None, pl.ds(0, WIN), pl.ds(0, WIN), None)
    project(halo[1], key_pad(n_rows), k_aug, vT, None, pl.ds(n_rows + WIN, WIN), pl.ds(n_rows + WIN, WIN), None)

    jj = lax.broadcasted_iota(jnp.int32, (WIN, BQ), 0)
    ii = lax.broadcasted_iota(jnp.int32, (WIN, BQ), 1)

    def pipeline(n_blocks, n_ch, keys, queries, values, window, finish, hooks=None):
        def score(b, h, c, mx):
            sc = jnp.dot(keys(b, h, c), queries(b, h), preferred_element_type=F32)
            if window and c == 0:
                sc = jnp.where(ii <= jj, sc, NEG)
            if window and c == n_ch - 1:
                sc = jnp.where(jj <= ii, sc, NEG)
            s_scr[h, pl.ds(c * BQ, BQ)] = sc
            top = jnp.max(sc.reshape(BQ // 8, 8, BQ), axis=0)
            return top if mx is None else jnp.maximum(mx, top)

        def first(b, h):
            mx = None
            for c in range(n_ch):
                mx = score(b, h, c, mx)
            m_scr[h] = mx

        def both(b, h, b2, h2):
            mx = jnp.max(m_scr[h], axis=0, keepdims=True)
            mx = finish(b, h, mx, None, None, True)
            nxt, ls, ac = None, None, None
            for c in range(n_ch):
                nxt = score(b2, h2, c, nxt)
                e = jnp.exp2(s_scr[h, pl.ds(c * BQ, BQ)] - mx)
                le = jnp.sum(e.reshape(BQ // 8, 8, BQ), axis=0)
                ls = le if ls is None else ls + le
                pv = jnp.dot(values(b, h, c), e.astype(BF16), preferred_element_type=F32)
                ac = pv if ac is None else ac + pv
            m_scr[h2] = nxt
            finish(b, h, mx, jnp.sum(ls, axis=0, keepdims=True), ac, False)

        def body(b, carry):
            for at, hook in (hooks or {}).items():
                pl.when(b == at)(hook)
            for h in range(n_heads):
                if h + 1 < n_heads:
                    both(b, h, b, h + 1)
                else:
                    both(b, h, jnp.minimum(b + 1, n_blocks - 1), 0)
            return carry

        first(0, 0)
        lax.fori_loop(0, n_blocks, body, 0)

    def cols_of(b):
        return pl.ds(pl.multiple_of(b * BQ, BQ), BQ)

    def rows_at(b, c, off=0):
        return pl.ds(pl.multiple_of(b * BQ + c * BQ + off, BQ), BQ)

    def window_done(b, h, mx, ls, ac, start):
        if start:
            return mx
        m_w[b, pl.ds(h, 1)] = mx
        l_w[b, pl.ds(h, 1)] = ls
        acc_w[b, pl.ds(h * hd, hd)] = ac

    pipeline(n_blk, 1 + 2 * WIN // BQ, lambda b, h, c: k_aug[h, rows_at(b, c)], lambda b, h: qT[h, :, cols_of(b)],
             lambda b, h, c: vT[pl.ds(h * hd, hd), rows_at(b, c)], True, window_done)

    for c in ag:
        c.wait_recv()
    n_half = n_x * n_tp
    agd = remote(xg.at[pl.ds(core * n_half, n_half)], xg.at[pl.ds(core * n_half, n_half)], agd_s.at[0], agd_r.at[0], {'sp': partner})
    agd_in = remote(xg.at[pl.ds((1 - core) * n_half, n_half)], xg.at[pl.ds((1 - core) * n_half, n_half)], agd_s.at[0], agd_r.at[0], {'sp': partner})
    agd.start()
    arrive(wf[0])
    start(wxb[0])
    start(wd[0])
    agd_in.wait_recv()
    gb = BQ // per
    for g in range(G // BQ):
        rows = xg[pl.ds(g * gb, gb)].reshape(BQ, x_ref.shape[1])
        cols = pl.ds(g * BQ, BQ)
        project(rows, jnp.zeros((BQ, hd), BF16), kg_aug, vgT, qgT, cols, cols, cols)

    gper = G // n_sp

    def second_piece():
        arrive(wy[1])
        start(wf[1])

    def gq_done(g, h, mx, ls, ac, start):
        if start:
            return mx
        for q in range(BQ // gper):
            cc = slice(q * gper, (q + 1) * gper)
            dst = g * (BQ // gper) + q
            part[dst, pl.ds(h * hd, hd)] = ac[:, cc]
            part[dst, pl.ds(width + h, 1)] = mx[:, cc]
            part[dst, pl.ds(width + 8 + h, 1)] = ls[:, cc]

    pipeline(G // BQ, n_rows // BQ, lambda b, h, c: k_aug[h, pl.ds(WIN + c * BQ, BQ)], lambda b, h: qgT[h, :, cols_of(b)],
             lambda b, h, c: vT[pl.ds(h * hd, hd), pl.ds(WIN + c * BQ, BQ)], False, gq_done, {1: second_piece})
    pt = [remote(part.at[sp(d)], part_recv.at[s], pt_s.at[d - 1], pt_r.at[d - 1], {'sp': sp(d)}) for d in range(1, n_sp)]
    for c in pt:
        c.start()
    def third_piece():
        arrive(wy[2])
        start(wf[2])
        start(wxa[2])

    def second_forward():
        arrive(wf[1])
        start(wd[1])

    def glob_done(b, h, mx, ls, ac, start):
        m_old = m_w[b, pl.ds(h, 1)]
        if start:
            return jnp.maximum(mx, m_old)
        alpha = jnp.exp2(m_old - mx)
        total = ls + l_w[b, pl.ds(h, 1)] * alpha
        acc_w[b, pl.ds(h * hd, hd)] = (ac + acc_w[b, pl.ds(h * hd, hd)] * alpha) / total

    pipeline(n_blk, G // BQ, lambda b, h, c: kg_aug[h, pl.ds(c * BQ, BQ)], lambda b, h: qT[h, :, cols_of(b)],
             lambda b, h, c: vgT[pl.ds(h * hd, hd), pl.ds(c * BQ, BQ)], False, glob_done, {1: third_piece, 4: second_forward})

    arrive(wf[2])
    start(wxb[2])
    start(wd[2])
    for c in pt:
        c.wait_recv()
    part_recv[s] = part[s]
    for h in range(n_heads):
        ms = part_recv[:, pl.ds(width + h, 1)]
        mx = jnp.max(ms, axis=0, keepdims=True)
        wt = jnp.exp2(ms - mx)
        den = jnp.sum(part_recv[:, pl.ds(width + 8 + h, 1)] * wt, axis=0)
        num = jnp.sum(part_recv[:, pl.ds(h * hd, hd)] * wt, axis=0)
        og_all[s, pl.ds(h * hd, hd)] = (num / den).astype(BF16)
    og = [remote(og_all.at[s], og_all.at[s], og_s.at[d - 1], og_r.at[d - 1], {'sp': sp(d)}) for d in range(1, n_sp)]
    for c in og:
        c.start()
    arrive(wxa_in[0])
    arrive(wxb_in[0])
    for c in og:
        c.wait_recv()
    og_ext[pl.ds(width, 16)] = jnp.ones((16, G), BF16)
    for d in range(n_sp):
        og_ext[pl.ds(0, width), pl.ds(d * gper, gper)] = og_all[d]

    chunk = n_rows // n_tp
    per_chunk = chunk // BQ
    a2a = []
    for p in range(per_chunk):
        def pick_block(ch, carry):
            b = ch * per_chunk + p
            pos = s * n_rows + b * BQ + lax.broadcasted_iota(jnp.int32, (BQ, G), 0)
            hot = (pos == gpos).astype(F32).astype(BF16)
            sel = lax.dot_general(og_ext[...], hot, NT, preferred_element_type=F32)
            o_loc[p, ch] = jnp.where(sel[width:width + 1] > 0.5, sel[:width], acc_w[b]).astype(BF16)
            return carry

        lax.fori_loop(0, n_tp, pick_block, 0)
        a2a.append([remote(o_loc.at[p, tp(-r)], o_in.at[p, r - 1], a2a_s.at[p, r - 1], a2a_r.at[p, r - 1], {'tp': tp(-r)}) for r in range(1, n_tp)])
        start(a2a[p])
    arrive(wxa_in[2])
    arrive(wxb_in[2])
    start(wd[3])

    def rows_of(d, p):
        return pl.ds(pl.multiple_of(tp(d) * chunk + p * BQ, BQ), BQ)

    first, first_in = [], []
    for p in range(2):
        for j, d in enumerate((-1, 1)):
            first.append(remote(y_ref.at[rows_of(0, p)], y_ref.at[rows_of(0, p)], y_s.at[2 * p + j], y_r.at[2 * p + j], {'tp': tp(d)}))
            first_in.append(remote(y_ref.at[rows_of(-d, p)], y_ref.at[rows_of(-d, p)], y_s.at[2 * p + j], y_r.at[2 * p + j], {'tp': tp(d)}))
    fwd = [remote(y_ref.at[rows_of(1, 0)], y_ref.at[rows_of(1, 0)], f_s.at[0], f_r.at[0], {'tp': tp(-1)}),
           remote(y_ref.at[rows_of(-1, 1)], y_ref.at[rows_of(-1, 1)], f_s.at[1], f_r.at[1], {'tp': tp(1)})]
    fwd_in = [remote(y_ref.at[rows_of(2, 0)], y_ref.at[rows_of(2, 0)], f_s.at[0], f_r.at[0], {'tp': tp(-1)}),
              remote(y_ref.at[rows_of(2, 1)], y_ref.at[rows_of(2, 1)], f_s.at[1], f_r.at[1], {'tp': tp(1)})]

    for p in range(2):
        arrive(a2a[p])
        if p == 0:
            for c in own:
                c.wait()
            for group in wd_in:
                arrive(group)
        mixed = jnp.zeros((BQ, D), F32)
        for r in range(n_tp):
            o_r = o_loc[p, t] if r == 0 else o_in[p, r - 1]
            w = wo_own[...] if r == 0 else wo_in[r - 1]
            mixed = mixed + lax.dot_general(o_r, w, TN, preferred_element_type=F32)
        hidden = (x_ref[rows_of(0, p)].astype(F32) + mixed).astype(BF16)
        down = jnp.zeros((BQ, D), F32)
        for r in range(n_tp):
            z = jnp.dot(hidden, w1_own[...] if r == 0 else w1_in[r - 1], preferred_element_type=F32)
            u = jax.nn.gelu(z, approximate=True).astype(BF16)
            down = down + jnp.dot(u, w2_own[...] if r == 0 else w2_in[r - 1], preferred_element_type=F32)
        y_ref[rows_of(0, p)] = (hidden.astype(F32) + down).astype(BF16)
        first[2 * p].start()
        first[2 * p + 1].start()
    first_in[0].wait_recv()
    fwd[0].start()
    first_in[3].wait_recv()
    fwd[1].start()
    first_in[1].wait_recv()
    first_in[2].wait_recv()
    arrive(fwd_in)
    for c in rs + halo_c + ag + [agd] + pt + og + sum(a2a + wy + wf + wxa + wxb + wd, []) + first + fwd:
        c.wait_send()


def solution(mesh):
    n_sp, n_tp = mesh.shape['sp'], mesh.shape['tp']

    def device_layer(tokens, glob_pos, w_query, w_key, w_value, w_out, w_up, w_down):
        n_rows, D = tokens.shape
        n_heads, hd = w_query.shape[1], w_query.shape[2]
        width = n_heads * hd
        G = glob_pos.shape[0]
        n_x = n_sp // 2
        per = G // (n_sp * n_tp)
        dims = (n_sp, n_tp, n_heads, hd)
        ext_rows = n_rows + 2 * WIN

        flat = lambda w: w.reshape(D, width)
        wqkv = jnp.concatenate([flat(w_query).T, flat(w_value).T, flat(w_key).T], axis=0)
        vm = pl.BlockSpec(memory_space=pltpu.VMEM)
        dma = pltpu.SemaphoreType.DMA
        n_blk = n_rows // BQ
        return pl.pallas_call(
            functools.partial(layer_kernel, dims),
            out_shape=jax.ShapeDtypeStruct((n_rows, D), BF16),
            in_specs=[vm] * 3 + [pl.BlockSpec(memory_space=pl.ANY)] * 3,
            out_specs=vm,
            scratch_shapes=[
                pltpu.VMEM(w_up.shape, BF16), pltpu.VMEM(w_down.shape, BF16), pltpu.VMEM((width, D), BF16),
                pltpu.VMEM((n_tp - 1,) + w_up.shape, BF16), pltpu.VMEM((n_tp - 1,) + w_down.shape, BF16), pltpu.VMEM((n_tp - 1, width, D), BF16),
                pltpu.VMEM((n_sp, per, D), BF16),
                pltpu.VMEM((2, WIN, D), BF16), pltpu.VMEM((n_sp, per, D), BF16), pltpu.VMEM((n_sp * n_tp, per, D), BF16),
                pltpu.VMEM((n_heads, n_rows, BQ), F32), pltpu.VMEM((n_heads, 8, BQ), F32),
                pltpu.VMEM((n_heads, 4 * hd, n_rows), BF16), pltpu.VMEM((n_heads, ext_rows, 4 * hd), BF16), pltpu.VMEM((width, ext_rows), BF16),
                pltpu.VMEM((n_heads, 4 * hd, G), BF16), pltpu.VMEM((n_heads, G, 4 * hd), BF16), pltpu.VMEM((width, G), BF16),
                pltpu.VMEM((n_blk, 8, BQ), F32), pltpu.VMEM((n_blk, 8, BQ), F32), pltpu.VMEM((n_blk, width, BQ), F32),
                pltpu.VMEM((n_sp, width + 16, G // n_sp), F32), pltpu.VMEM((n_sp, width + 16, G // n_sp), F32),
                pltpu.VMEM((n_sp, width, G // n_sp), BF16), pltpu.VMEM((width + 16, G), BF16),
                pltpu.VMEM((2, n_tp, width, BQ), BF16), pltpu.VMEM((2, n_tp - 1, width, BQ), BF16),
                dma((2,)), dma((2,)), dma((n_sp - 1,)), dma((n_sp - 1,)), dma((n_x * n_tp - 1,)), dma((n_x * n_tp - 1,)),
                dma((1,)), dma((1,)), dma((n_sp - 1,)), dma((n_sp - 1,)), dma((n_sp - 1,)), dma((n_sp - 1,)),
                dma((2, n_tp - 1)), dma((2, n_tp - 1)),
                dma((3, 2, 3)), dma((3, 2, 3)), dma((3, 3)), dma((3, 3)), dma((3, 3)), dma((3, 3)), dma((4, 2)), dma((4, 2)),
                dma((4,)), dma((4,)), dma((2,)), dma((2,)), dma((3,)),
            ],
            compiler_params=pltpu.CompilerParams(collective_id=0, has_side_effects=True, vmem_limit_bytes=62 * 1024 * 1024),
            name='layer',
        )(tokens, wqkv, glob_pos.reshape(2 * n_tp, n_x * per), w_up, w_down, w_out.reshape(width, D))

    row_spec = P(('dp', 'sp'), None)
    head_spec = P(None, 'tp', None)
    in_specs = (row_spec, P('dp'), head_spec, head_spec, head_spec, P('tp', None, None), P(None, 'tp'), P('tp', None))
    return jax.shard_map(device_layer, mesh=mesh, in_specs=in_specs, out_specs=row_spec, check_vma=False)
```

```python
import functools
import math

import jax
import jax.numpy as jnp
from jax import lax
from jax.experimental import pallas as pl
from jax.experimental.pallas import tpu as pltpu
from jax.sharding import PartitionSpec as P

WIN = 256
NEG = -1e38
LOG2E = math.log2(math.e)
BQ = 256
F32 = jnp.float32
BF16 = jnp.bfloat16
MESH = pl.DeviceIdType.MESH
NT = (((1,), (1,)), ((), ()))
TN = (((0,), (0,)), ((), ()))


def remote(src, dst, send, recv, where):
    return pltpu.make_async_remote_copy(src_ref=src, dst_ref=dst, send_sem=send, recv_sem=recv, device_id=where, device_id_type=MESH)


def layer_kernel(dims, x_ref, wqkv_ref, gpos_ref, w1_ref, w2_ref, wo_ref,
                 y_ref,
                 w1_own, w2_own, wo_own, w1_in, w2_in, wo_in, pick, halo, rs_recv, xg, s_scr, m_scr, qT, k_aug, vT, qgT, kg_aug, vgT, m_w, l_w, acc_w, part, part_recv,
                 og_all, og_ext, o_loc, o_in,
                 halo_s, halo_r, rs_s, rs_r, ag_s, ag_r, agd_s, agd_r, pt_s, pt_r, og_s, og_r, a2a_s, a2a_r,
                 wy_s, wy_r, wf_s, wf_r, wx_s, wx_r, wd_s, wd_r, y_s, y_r, f_s, f_r, own_s):
    n_sp, n_tp, n_heads, hd = dims
    n_rows, D = x_ref.shape
    width = n_heads * hd
    n_x = n_sp // 2
    n_blk = n_rows // BQ
    s = lax.axis_index('sp')
    t = lax.axis_index('tp')
    core = s % 2
    chip = s // 2
    G = gpos_ref.shape[0] * gpos_ref.shape[1]
    gpos = jnp.concatenate([gpos_ref[pl.ds(i, 1)] for i in range(gpos_ref.shape[0])], axis=1)
    per = G // (n_sp * n_tp)
    def sp(d):
        return (s + d + n_sp) % n_sp

    def tp(d):
        return (t + d + n_tp) % n_tp

    own = [pltpu.make_async_copy(a, b, own_s.at[i]) for i, (a, b) in enumerate(((wo_ref, wo_own), (w1_ref, w1_own), (w2_ref, w2_own)))]
    for c in own:
        c.start()

    bar = pltpu.get_barrier_semaphore()
    n_peers = 0
    for d in range(1, n_sp):
        pl.semaphore_signal(bar, inc=1, device_id={'sp': sp(d)}, device_id_type=MESH)
        n_peers += 1
    for dt in range(1, n_tp):
        for dx in range(n_x):
            pl.semaphore_signal(bar, inc=1, device_id={'sp': sp(2 * dx), 'tp': tp(dt)}, device_id_type=MESH)
            n_peers += 1
    pl.semaphore_wait(bar, n_peers)

    halo_c = [remote(x_ref.at[pl.ds(n_rows - WIN, WIN)], halo.at[0], halo_s.at[0], halo_r.at[0], {'sp': sp(1)}),
              remote(x_ref.at[pl.ds(0, WIN)], halo.at[1], halo_s.at[1], halo_r.at[1], {'sp': sp(-1)})]
    for c in halo_c:
        c.start()

    weights = [(wo_ref, wo_in, 2 * width // n_sp, 2), (w1_ref, w1_in, D // n_sp, 1), (w2_ref, w2_in, D // n_sp, 1)]

    def wslice(piece, size, share):
        return pl.ds(pl.multiple_of((((piece + n_sp) % n_sp) // share) * size, size), size)

    wy, wf, wxa, wxa_in, wxb, wxb_in, wd, wd_in = [], [], [], [], [], [], [], []
    partner = 2 * chip + 1 - core
    for p in range(3):
        gy, gf, ga, ga_in, gb2, gb_in = [], [], [], [], [], []
        d2 = {'sp': sp(2 - 2 * p)}
        for a, (w, win, size, share) in enumerate(weights):
            rows = wslice(s + 2 * p, size, share)
            come = wslice(s - 2, size, share)
            for k, (d, slot) in enumerate(((-1, 0), (1, 2))):
                gy.append(remote(w.at[rows], win.at[slot, rows], wy_s.at[p, k, a], wy_r.at[p, k, a], {'tp': tp(d)}))
            d, slot = ((-1, 0), (-1, 0), (1, 2))[a]
            gf.append(remote(win.at[slot, rows], win.at[1, rows], wf_s.at[p, a], wf_r.at[p, a], {'tp': tp(d)}))
            if p == (0, 0, 2)[a]:
                for slot in (0, 2):
                    ga.append(remote(win.at[slot, rows], win.at[slot, rows], wx_s.at[slot, a], wx_r.at[slot, a], d2))
                    ga_in.append(remote(win.at[slot, come], win.at[slot, come], wx_s.at[slot, a], wx_r.at[slot, a], d2))
                gb2.append(remote(win.at[1, rows], win.at[1, rows], wx_s.at[1, a], wx_r.at[1, a], d2))
                gb_in.append(remote(win.at[1, come], win.at[1, come], wx_s.at[1, a], wx_r.at[1, a], d2))
        wy.append(gy)
        wf.append(gf)
        wxa.append(ga)
        wxa_in.append(ga_in)
        wxb.append(gb2)
        wxb_in.append(gb_in)
    for j in range(4):
        gd, gd_in = [], []
        for a, (w, win, size, share) in enumerate(weights[1:]):
            rows, come = wslice(s + 2 * j, size, share), wslice(partner + 2 * j, size, share)
            gd.append(remote(win.at[:, rows], win.at[:, rows], wd_s.at[j, a], wd_r.at[j, a], {'sp': partner}))
            gd_in.append(remote(win.at[:, come], win.at[:, come], wd_s.at[j, a], wd_r.at[j, a], {'sp': partner}))
        wd.append(gd)
        wd_in.append(gd_in)

    def start(copies):
        for c in copies:
            c.start()

    def arrive(copies):
        for c in copies:
            c.wait_recv()

    start(wy[0])

    slots = jnp.concatenate([gpos_ref[pl.ds(c * n_tp + t, 1)] for c in range(2)], axis=1)
    slots = jnp.transpose(jnp.broadcast_to(slots, (8, n_sp * per)))[:, :1]
    hot = (s * n_rows + lax.broadcasted_iota(jnp.int32, (n_sp * per, n_rows), 1) == slots).astype(F32).astype(BF16)
    pick[...] = jnp.dot(hot, x_ref[...], preferred_element_type=F32).astype(BF16).reshape(n_sp, per, D)

    def slot_block(dev):
        return (dev % 2) * n_x + dev // 2

    rs = [remote(pick.at[slot_block(sp(d))], rs_recv.at[s], rs_s.at[d - 1], rs_r.at[d - 1], {'sp': sp(d)}) for d in range(1, n_sp)]
    start(rs)

    def project(rows, pad, kdst, vdst, qdst, kdst_row, vcol, qcol):
        qv = lax.dot_general(wqkv_ref[pl.ds(0, 2 * width)], rows, NT, preferred_element_type=F32).astype(BF16)
        kk = lax.dot_general(rows, wqkv_ref[pl.ds(2 * width, width)], NT, preferred_element_type=F32).astype(BF16)
        vdst[:, vcol] = qv[width:]
        for h in range(n_heads):
            kh = kk[:, h * hd:(h + 1) * hd]
            kdst[h, kdst_row, pl.ds(0, 2 * hd)] = jnp.concatenate([kh, kh], axis=1)
            kdst[h, kdst_row, pl.ds(2 * hd, 2 * hd)] = jnp.concatenate([kh, pad], axis=1)
        if qdst is not None:
            rest = qv[:width].astype(F32) * (LOG2E / math.sqrt(hd))
            for i in range(3):
                cut = rest.astype(BF16)
                rest = rest - cut.astype(F32)
                for h in range(n_heads):
                    qdst[h, pl.ds(i * hd, hd), qcol] = cut[h * hd:(h + 1) * hd]

    mark = jnp.where(lax.broadcasted_iota(jnp.int32, (G, hd), 1) == 0, NEG, 0.0).astype(BF16)

    def key_pad(off):
        pos = s * n_rows + off + lax.broadcasted_iota(jnp.int32, (BQ, G), 0)
        pad = jnp.dot((pos == gpos).astype(F32).astype(BF16), mark, preferred_element_type=F32)
        at = s * n_rows + off + lax.broadcasted_iota(jnp.int32, (BQ, hd), 0)
        lane = lax.broadcasted_iota(jnp.int32, (BQ, hd), 1)
        return jnp.where((lane == 0) & ((at < 0) | (at >= n_rows * n_sp)), NEG, pad).astype(BF16)

    def proj_block(b, carry):
        base = pl.multiple_of(b * BQ, BQ)
        ext = pl.multiple_of(b * BQ + WIN, BQ)
        project(x_ref[pl.ds(base, BQ)], key_pad(base), k_aug, vT, qT, pl.ds(ext, BQ), pl.ds(ext, BQ), pl.ds(base, BQ))
        return carry

    flag_row = (lax.broadcasted_iota(jnp.int32, (hd, BQ), 0) == 0).astype(F32).astype(BF16)
    for h in range(n_heads):
        for b in range(n_blk):
            qT[h, pl.ds(3 * hd, hd), pl.ds(b * BQ, BQ)] = flag_row
        qgT[h, pl.ds(3 * hd, hd)] = jnp.zeros((hd, G), BF16)
    lax.fori_loop(0, n_blk, proj_block, 0)

    for c in rs:
        c.wait_recv()
    mine = core * (n_x * n_tp) + t * n_x + chip
    rs_recv[s] = pick[core * n_x + chip]
    xg[mine] = jnp.sum(rs_recv[...].astype(F32), axis=0).astype(BF16)
    ag = []
    for dt in range(n_tp):
        for dx in range(n_x):
            if dt or dx:
                j = dt * n_x + dx - 1
                ag.append(remote(xg.at[mine], xg.at[mine], ag_s.at[j], ag_r.at[j], {'sp': sp(2 * dx), 'tp': tp(dt)}))
    start(ag)
    arrive(wy[0])
    start(wf[0])
    start(wxa[0])
    start(wy[1])
    start(wy[2])
    arrive(halo_c)
    project(halo[0], key_pad(-WIN), k_aug, vT, None, pl.ds(0, WIN), pl.ds(0, WIN), None)
    project(halo[1], key_pad(n_rows), k_aug, vT, None, pl.ds(n_rows + WIN, WIN), pl.ds(n_rows + WIN, WIN), None)

    jj = lax.broadcasted_iota(jnp.int32, (WIN, BQ), 0)
    ii = lax.broadcasted_iota(jnp.int32, (WIN, BQ), 1)

    def pipeline(n_blocks, n_ch, keys, queries, values, window, finish, hooks=None, after=None):
        def score(b, h, c, mx):
            sc = jnp.dot(keys(b, h, c), queries(b, h), preferred_element_type=F32)
            if window and c == 0:
                sc = jnp.where(ii <= jj, sc, NEG)
            if window and c == n_ch - 1:
                sc = jnp.where(jj <= ii, sc, NEG)
            s_scr[h, pl.ds(c * BQ, BQ)] = sc
            top = jnp.max(sc.reshape(BQ // 8, 8, BQ), axis=0)
            return top if mx is None else jnp.maximum(mx, top)

        def first(b, h):
            mx = None
            for c in range(n_ch):
                mx = score(b, h, c, mx)
            m_scr[h] = mx

        def both(b, h, b2, h2):
            mx = jnp.max(m_scr[h], axis=0, keepdims=True)
            mx = finish(b, h, mx, None, None, True)
            nxt, ls, ac = None, None, None
            for c in range(n_ch):
                nxt = score(b2, h2, c, nxt)
                e = jnp.exp2(s_scr[h, pl.ds(c * BQ, BQ)] - mx)
                le = jnp.sum(e.reshape(BQ // 8, 8, BQ), axis=0)
                ls = le if ls is None else ls + le
                pv = jnp.dot(values(b, h, c), e.astype(BF16), preferred_element_type=F32)
                ac = pv if ac is None else ac + pv
            m_scr[h2] = nxt
            finish(b, h, mx, jnp.sum(ls, axis=0, keepdims=True), ac, False)

        def body(b, carry):
            for at, hook in (hooks or {}).items():
                pl.when(b == at)(hook)
            for h in range(n_heads):
                if h + 1 < n_heads:
                    both(b, h, b, h + 1)
                else:
                    both(b, h, jnp.minimum(b + 1, n_blocks - 1), 0)
            if after is not None:
                after(b)
            return carry

        first(0, 0)
        lax.fori_loop(0, n_blocks, body, 0)

    def cols_of(b):
        return pl.ds(pl.multiple_of(b * BQ, BQ), BQ)

    def rows_at(b, c, off=0):
        return pl.ds(pl.multiple_of(b * BQ + c * BQ + off, BQ), BQ)

    def window_done(b, h, mx, ls, ac, start):
        if start:
            return mx
        m_w[b, pl.ds(h, 1)] = mx
        l_w[b, pl.ds(h, 1)] = ls
        acc_w[b, pl.ds(h * hd, hd)] = ac

    pipeline(n_blk, 1 + 2 * WIN // BQ, lambda b, h, c: k_aug[h, rows_at(b, c)], lambda b, h: qT[h, :, cols_of(b)],
             lambda b, h, c: vT[pl.ds(h * hd, hd), rows_at(b, c)], True, window_done)

    for c in ag:
        c.wait_recv()
    n_half = n_x * n_tp
    agd = remote(xg.at[pl.ds(core * n_half, n_half)], xg.at[pl.ds(core * n_half, n_half)], agd_s.at[0], agd_r.at[0], {'sp': partner})
    agd_in = remote(xg.at[pl.ds((1 - core) * n_half, n_half)], xg.at[pl.ds((1 - core) * n_half, n_half)], agd_s.at[0], agd_r.at[0], {'sp': partner})
    agd.start()
    arrive(wf[0])
    start(wxb[0])
    start(wd[0])
    agd_in.wait_recv()
    gb = BQ // per
    for g in range(G // BQ):
        rows = xg[pl.ds(g * gb, gb)].reshape(BQ, x_ref.shape[1])
        cols = pl.ds(g * BQ, BQ)
        project(rows, jnp.zeros((BQ, hd), BF16), kg_aug, vgT, qgT, cols, cols, cols)

    gper = G // n_sp

    def send_part(g):
        for q in range(BQ // gper):
            dst = g * (BQ // gper) + q

            @pl.when(dst != s)
            def _():
                j = (dst - s + n_sp) % n_sp - 1
                remote(part.at[dst], part_recv.at[s], pt_s.at[j], pt_r.at[j], {'sp': dst}).start()

    def second_piece():
        arrive(wy[1])
        start(wf[1])

    def gq_done(g, h, mx, ls, ac, start):
        if start:
            return mx
        for q in range(BQ // gper):
            cc = slice(q * gper, (q + 1) * gper)
            dst = g * (BQ // gper) + q
            part[dst, pl.ds(h * hd, hd)] = ac[:, cc]
            part[dst, pl.ds(width + h, 1)] = mx[:, cc]
            part[dst, pl.ds(width + 8 + h, 1)] = ls[:, cc]

    pipeline(G // BQ, n_rows // BQ, lambda b, h, c: k_aug[h, pl.ds(WIN + c * BQ, BQ)], lambda b, h: qgT[h, :, cols_of(b)],
             lambda b, h, c: vT[pl.ds(h * hd, hd), pl.ds(WIN + c * BQ, BQ)], False, gq_done, {1: second_piece}, send_part)
    pt = [remote(part.at[sp(d)], part_recv.at[s], pt_s.at[d - 1], pt_r.at[d - 1], {'sp': sp(d)}) for d in range(1, n_sp)]
    def third_piece():
        arrive(wy[2])
        start(wf[2])
        start(wxa[2])

    def second_forward():
        arrive(wf[1])
        start(wd[1])

    def glob_done(b, h, mx, ls, ac, start):
        m_old = m_w[b, pl.ds(h, 1)]
        if start:
            return jnp.maximum(mx, m_old)
        alpha = jnp.exp2(m_old - mx)
        total = ls + l_w[b, pl.ds(h, 1)] * alpha
        acc_w[b, pl.ds(h * hd, hd)] = (ac + acc_w[b, pl.ds(h * hd, hd)] * alpha) / total

    pipeline(n_blk, G // BQ, lambda b, h, c: kg_aug[h, pl.ds(c * BQ, BQ)], lambda b, h: qT[h, :, cols_of(b)],
             lambda b, h, c: vgT[pl.ds(h * hd, hd), pl.ds(c * BQ, BQ)], False, glob_done, {1: third_piece, 4: second_forward})

    arrive(wf[2])
    start(wxb[2])
    start(wd[2])
    for c in pt:
        c.wait_recv()
    part_recv[s] = part[s]
    for h in range(n_heads):
        ms = part_recv[:, pl.ds(width + h, 1)]
        mx = jnp.max(ms, axis=0, keepdims=True)
        wt = jnp.exp2(ms - mx)
        den = jnp.sum(part_recv[:, pl.ds(width + 8 + h, 1)] * wt, axis=0)
        num = jnp.sum(part_recv[:, pl.ds(h * hd, hd)] * wt, axis=0)
        og_all[s, pl.ds(h * hd, hd)] = (num / den).astype(BF16)
    og = [remote(og_all.at[s], og_all.at[s], og_s.at[d - 1], og_r.at[d - 1], {'sp': sp(d)}) for d in range(1, n_sp)]
    for c in og:
        c.start()
    arrive(wxa_in[0])
    arrive(wxb_in[0])
    for c in og:
        c.wait_recv()
    og_ext[pl.ds(width, 16)] = jnp.ones((16, G), BF16)
    for d in range(n_sp):
        og_ext[pl.ds(0, width), pl.ds(d * gper, gper)] = og_all[d]

    chunk = n_rows // n_tp
    per_chunk = chunk // BQ
    a2a = []
    for p in range(per_chunk):
        def pick_block(ch, carry):
            b = ch * per_chunk + p
            pos = s * n_rows + b * BQ + lax.broadcasted_iota(jnp.int32, (BQ, G), 0)
            hot = (pos == gpos).astype(F32).astype(BF16)
            sel = lax.dot_general(og_ext[...], hot, NT, preferred_element_type=F32)
            o_loc[p, ch] = jnp.where(sel[width:width + 1] > 0.5, sel[:width], acc_w[b]).astype(BF16)
            return carry

        lax.fori_loop(0, n_tp, pick_block, 0)
        a2a.append([remote(o_loc.at[p, tp(-r)], o_in.at[p, r - 1], a2a_s.at[p, r - 1], a2a_r.at[p, r - 1], {'tp': tp(-r)}) for r in range(1, n_tp)])
        start(a2a[p])
    arrive(wxa_in[2])
    arrive(wxb_in[2])
    start(wd[3])

    def rows_of(d, p):
        return pl.ds(pl.multiple_of(tp(d) * chunk + p * BQ, BQ), BQ)

    first, first_in = [], []
    for p in range(2):
        for j, d in enumerate((-1, 1)):
            first.append(remote(y_ref.at[rows_of(0, p)], y_ref.at[rows_of(0, p)], y_s.at[2 * p + j], y_r.at[2 * p + j], {'tp': tp(d)}))
            first_in.append(remote(y_ref.at[rows_of(-d, p)], y_ref.at[rows_of(-d, p)], y_s.at[2 * p + j], y_r.at[2 * p + j], {'tp': tp(d)}))
    fwd = [remote(y_ref.at[rows_of(1, 0)], y_ref.at[rows_of(1, 0)], f_s.at[0], f_r.at[0], {'tp': tp(-1)}),
           remote(y_ref.at[rows_of(-1, 1)], y_ref.at[rows_of(-1, 1)], f_s.at[1], f_r.at[1], {'tp': tp(1)})]
    fwd_in = [remote(y_ref.at[rows_of(2, 0)], y_ref.at[rows_of(2, 0)], f_s.at[0], f_r.at[0], {'tp': tp(-1)}),
              remote(y_ref.at[rows_of(2, 1)], y_ref.at[rows_of(2, 1)], f_s.at[1], f_r.at[1], {'tp': tp(1)})]

    for p in range(2):
        arrive(a2a[p])
        if p == 0:
            for c in own:
                c.wait()
            for group in wd_in:
                arrive(group)
        mixed = jnp.zeros((BQ, D), F32)
        for r in range(n_tp):
            o_r = o_loc[p, t] if r == 0 else o_in[p, r - 1]
            w = wo_own[...] if r == 0 else wo_in[r - 1]
            mixed = mixed + lax.dot_general(o_r, w, TN, preferred_element_type=F32)
        hidden = (x_ref[rows_of(0, p)].astype(F32) + mixed).astype(BF16)
        down = jnp.zeros((BQ, D), F32)
        for r in range(n_tp):
            z = jnp.dot(hidden, w1_own[...] if r == 0 else w1_in[r - 1], preferred_element_type=F32)
            u = jax.nn.gelu(z, approximate=True).astype(BF16)
            down = down + jnp.dot(u, w2_own[...] if r == 0 else w2_in[r - 1], preferred_element_type=F32)
        y_ref[rows_of(0, p)] = (hidden.astype(F32) + down).astype(BF16)
        first[2 * p].start()
        first[2 * p + 1].start()
    first_in[0].wait_recv()
    fwd[0].start()
    first_in[3].wait_recv()
    fwd[1].start()
    first_in[1].wait_recv()
    first_in[2].wait_recv()
    arrive(fwd_in)
    for c in rs + halo_c + ag + [agd] + pt + og + sum(a2a + wy + wf + wxa + wxb + wd, []) + first + fwd:
        c.wait_send()


def solution(mesh):
    n_sp, n_tp = mesh.shape['sp'], mesh.shape['tp']

    def device_layer(tokens, glob_pos, w_query, w_key, w_value, w_out, w_up, w_down):
        n_rows, D = tokens.shape
        n_heads, hd = w_query.shape[1], w_query.shape[2]
        width = n_heads * hd
        G = glob_pos.shape[0]
        n_x = n_sp // 2
        per = G // (n_sp * n_tp)
        dims = (n_sp, n_tp, n_heads, hd)
        ext_rows = n_rows + 2 * WIN

        flat = lambda w: w.reshape(D, width)
        wqkv = jnp.concatenate([flat(w_query).T, flat(w_value).T, flat(w_key).T], axis=0)
        vm = pl.BlockSpec(memory_space=pltpu.VMEM)
        dma = pltpu.SemaphoreType.DMA
        n_blk = n_rows // BQ
        return pl.pallas_call(
            functools.partial(layer_kernel, dims),
            out_shape=jax.ShapeDtypeStruct((n_rows, D), BF16),
            in_specs=[vm] * 3 + [pl.BlockSpec(memory_space=pl.ANY)] * 3,
            out_specs=vm,
            scratch_shapes=[
                pltpu.VMEM(w_up.shape, BF16), pltpu.VMEM(w_down.shape, BF16), pltpu.VMEM((width, D), BF16),
                pltpu.VMEM((n_tp - 1,) + w_up.shape, BF16), pltpu.VMEM((n_tp - 1,) + w_down.shape, BF16), pltpu.VMEM((n_tp - 1, width, D), BF16),
                pltpu.VMEM((n_sp, per, D), BF16),
                pltpu.VMEM((2, WIN, D), BF16), pltpu.VMEM((n_sp, per, D), BF16), pltpu.VMEM((n_sp * n_tp, per, D), BF16),
                pltpu.VMEM((n_heads, n_rows, BQ), F32), pltpu.VMEM((n_heads, 8, BQ), F32),
                pltpu.VMEM((n_heads, 4 * hd, n_rows), BF16), pltpu.VMEM((n_heads, ext_rows, 4 * hd), BF16), pltpu.VMEM((width, ext_rows), BF16),
                pltpu.VMEM((n_heads, 4 * hd, G), BF16), pltpu.VMEM((n_heads, G, 4 * hd), BF16), pltpu.VMEM((width, G), BF16),
                pltpu.VMEM((n_blk, 8, BQ), F32), pltpu.VMEM((n_blk, 8, BQ), F32), pltpu.VMEM((n_blk, width, BQ), F32),
                pltpu.VMEM((n_sp, width + 16, G // n_sp), F32), pltpu.VMEM((n_sp, width + 16, G // n_sp), F32),
                pltpu.VMEM((n_sp, width, G // n_sp), BF16), pltpu.VMEM((width + 16, G), BF16),
                pltpu.VMEM((2, n_tp, width, BQ), BF16), pltpu.VMEM((2, n_tp - 1, width, BQ), BF16),
                dma((2,)), dma((2,)), dma((n_sp - 1,)), dma((n_sp - 1,)), dma((n_x * n_tp - 1,)), dma((n_x * n_tp - 1,)),
                dma((1,)), dma((1,)), dma((n_sp - 1,)), dma((n_sp - 1,)), dma((n_sp - 1,)), dma((n_sp - 1,)),
                dma((2, n_tp - 1)), dma((2, n_tp - 1)),
                dma((3, 2, 3)), dma((3, 2, 3)), dma((3, 3)), dma((3, 3)), dma((3, 3)), dma((3, 3)), dma((4, 2)), dma((4, 2)),
                dma((4,)), dma((4,)), dma((2,)), dma((2,)), dma((3,)),
            ],
            compiler_params=pltpu.CompilerParams(collective_id=0, has_side_effects=True, vmem_limit_bytes=62 * 1024 * 1024),
            name='layer',
        )(tokens, wqkv, glob_pos.reshape(2 * n_tp, n_x * per), w_up, w_down, w_out.reshape(width, D))

    row_spec = P(('dp', 'sp'), None)
    head_spec = P(None, 'tp', None)
    in_specs = (row_spec, P('dp'), head_spec, head_spec, head_spec, P('tp', None, None), P(None, 'tp'), P('tp', None))
    return jax.shard_map(device_layer, mesh=mesh, in_specs=in_specs, out_specs=row_spec, check_vma=False)
```
